512 devices in a mesh: replica: 32 (over z, x_hi, core), shard: 16 (over y, x_lo).
Axes of the slice: x: 4 (x_hi: 2, x_lo: 2; x = x_hi * 2 + x_lo), y: 8, z: 8, core: 2. Of those that a mesh axis runs over, the one named last changes fastest.
Arguments:
- local_weights: bfloat16 [32, 8192, 512], P('replica', 'shard'), may hold values from -1.3258252 to 1.3258252
- outer_base: bfloat16 [8192, 512], P('shard'), may hold values from -0.0625 to 0.0625
- momentum: bfloat16 [8192, 512], P('shard', 'replica'), may hold values from -0.06591797 to 0.06591797
- error_feedback: bfloat16 [32, 8192, 512], P('replica', 'shard'), may hold values from -0.032958984 to 0.032958984
- q_start: float32 [512, 32], replicated, may hold values from -6 to 6
- tokens: bfloat16 [32, 2048, 8192], P('replica', None, 'shard'), may hold values from -6 to 6
Outputs:
- new_base: bfloat16 [8192, 512], P('shard')
- new_momentum: bfloat16 [8192, 512], P('shard', 'replica')
- new_error: bfloat16 [32, 8192, 512], P('replica', 'shard')
- key_rows: bfloat16 [32, 2048, 512], P('replica', 'shard')
The draws below stay inside these ranges and needn't reach their ends.
All inputs are finite; a program needn't handle non-finite values.
Results may differ from the reference program's by a relative error of at most 0.0065.
Values may be sent and summed in bfloat16 or wider, within the bound.
No kernel may reach another device: no remote copies, remote signals or barrier semaphores. Data moves between devices by JAX's collectives and lax.ppermute only.
A program may use at most 64 MiB of HBM per device.

```python
import jax
import jax.numpy as jnp
from jax import lax

D = 8192
KV = 512
RANK = 32
TOKENS = 2048
REPLICAS = 32


def draw_local_weights(key, part):
    key_noise = jax.random.fold_in(key, 11)
    key_rows = jax.random.fold_in(key, 12)
    key_cols = jax.random.fold_in(key, 13)
    noise_val = jax.random.normal(key_noise, (REPLICAS, D, KV), jnp.float32)
    noise_val = jnp.clip(noise_val, -4.0, 4.0)
    rise_rows = 3.0 ** (jnp.arange(D, dtype=jnp.float32) / D)
    row_spread = 10.0 ** jax.random.uniform(key_rows, (D,), jnp.float32)
    col_spread = 10.0 ** jax.random.uniform(key_cols, (KV,), jnp.float32)
    scaled = noise_val * (rise_rows * row_spread)[None, :, None] * col_spread[None, None, :]
    return (scaled * (0.1 * D ** (-0.5))).astype(jnp.bfloat16)


def shard_levels(stream_key, shape, pieces, smallest, largest):
    factor_of, own = 1.0, jax.random.fold_in(stream_key, 6)
    for axis_at, shards_of in pieces:
        heights = jnp.exp(jax.random.uniform(jax.random.fold_in(own, axis_at), (shards_of,), jnp.float32, smallest / len(pieces), largest / len(pieces)))
        factor_of = factor_of * jnp.repeat(heights, shape[axis_at] // shards_of).reshape([-1 if axis == axis_at else 1 for axis in range(len(shape))])
    return factor_of


def gaussian(own_key, dims, width, limit, pieces=(), kind=jnp.bfloat16):
    result = jax.random.normal(own_key, dims, jnp.float32) * width
    if len(pieces) > 0:
        result = shard_levels(own_key, dims, pieces, -0.22, 0.18) * result
    return jnp.clip(result, min=-limit, max=limit).astype(kind)


def setup_inputs(seed: int = 0) -> dict:
    key_list = jax.random.split(jax.random.key(seed), 7)
    return {
        "local_weights": draw_local_weights(jax.random.fold_in(key_list[6], 71), 0),
        "outer_base": gaussian(key_list[1], (D, KV), D ** -0.5, 0.0625, ((0, 16),)),
        "momentum": gaussian(key_list[2], (D, KV), (D ** -0.5), 0.06591797, ((0, 16), (1, 32))),
        "error_feedback": gaussian(key_list[3], (REPLICAS, D, KV), (0.5 * D ** -0.5), 0.032958984, ((0, 32), (1, 16))),
        "q_start": gaussian(key_list[4], (KV, RANK), 1.0, 6.0, (), jnp.float32),
        "tokens": gaussian(key_list[5], (REPLICAS, TOKENS, D), 1.0, 6.0, ((0, 32), (2, 16))),
    }


outer_mu = 0.9
outer_rate = 0.7

def reference(local_weights, outer_base, momentum, error_feedback, q_start, tokens):
    highest = lax.Precision.HIGHEST
    pseudo = outer_base.astype(jnp.float32)[None] - local_weights.astype(jnp.float32) + error_feedback.astype(jnp.float32)
    p_mean = jnp.einsum('rdk,kq->dq', pseudo, q_start, precision=highest) / REPLICAS
    gram = jnp.dot(p_mean.T, p_mean, precision=highest)
    factor_low = jnp.linalg.cholesky(gram)
    basis = jax.scipy.linalg.solve_triangular(factor_low, p_mean.T, lower=True).T
    q_mean = jnp.einsum('rdk,dq->kq', pseudo, basis, precision=highest) / REPLICAS
    update = jnp.dot(basis, q_mean.T, precision=highest)
    new_error = (pseudo - update[None]).astype(jnp.bfloat16)
    moment = outer_mu * momentum.astype(jnp.float32) + update
    new_base = (outer_base.astype(jnp.float32) - outer_rate * (outer_mu * moment + update)).astype(jnp.bfloat16)

    def project(token_block):
        return jnp.dot(token_block.astype(jnp.float32), new_base.astype(jnp.float32), preferred_element_type=jnp.float32).astype(jnp.bfloat16)
    key_rows = lax.map(project, tokens)
    return (new_base, moment.astype(jnp.bfloat16), new_error, key_rows)
```

```python
import functools

import jax
import jax.numpy as jnp
from jax import lax
from jax.experimental import pallas as pl
from jax.experimental.pallas import tpu as pltpu
from jax.sharding import Mesh, PartitionSpec as P

outer_mu = 0.9
outer_rate = 0.7
own_mom = outer_rate * outer_mu * outer_mu
own_upd = outer_rate * (outer_mu + 1.0)

chips = ("z", "xh")
peers = ("core", "z", "xh")
shard = ("y2", "y1", "y0", "xl")
f32, bf16 = jnp.float32, jnp.bfloat16
highest = lax.Precision.HIGHEST


def swap(x, axis):
    return lax.ppermute(x, axis, [(0, 1), (1, 0)])


def exchange(x, axis):
    return lax.all_to_all(x, axis, 0, 0, tiled=True)


def copy_for_each(x, axis):
    return exchange(jnp.broadcast_to(x, (lax.axis_size(axis), *x.shape)), axis)


def pick(x, at, dim):
    return lax.dynamic_index_in_dim(x, at, dim, keepdims=False)


def halve(x, axis, dim):
    me = lax.axis_index(axis)
    other = swap(pick(x, 1 - me, dim).astype(bf16), axis)
    return pick(x, me, dim) + other.astype(f32)


def dot(a, b, dims, precision=None):
    return lax.dot_general(
        a, b, (dims, ((), ())), precision=precision, preferred_element_type=f32
    )


def lane_group(shape, rank):
    return lax.broadcasted_iota(jnp.int32, shape, 1) // rank


def moments(first_ref, q_ref, out_ref, *, own, rank, replicas):
    mean = jnp.sum(first_ref[:, :own].astype(f32), axis=0) * (1.0 / replicas)
    p = dot(mean, q_ref[...], ((1,), (0,)), highest)
    group = lane_group(p.shape, rank)
    p_at = [jnp.where(group == i, p, 0.0) for i in range(4)]
    upper = dot(p_at[0], p_at[1], ((0,), (0,)), highest)
    lower = dot(p_at[0], p_at[2], ((0,), (0,)), highest)
    same = p_at[0] + upper[:own] + lower[own : 2 * own]
    q_rows = dot(mean, p_at[3], ((0,), (0,)), highest)
    out_ref[...] = q_rows.reshape(out_ref.shape) + same[None]


def token_products(second_ref, tokens_ref, out_ref, *, own, rank):
    peers_, rows_, lanes = second_ref.shape
    shards = out_ref.shape[0]
    block = tokens_ref.shape[0] // shards
    step = block // 4
    second = second_ref[...]
    sums = jnp.sum(second, axis=0)
    flat = second.reshape(peers_ * rows_, lanes)
    p = jnp.where(lane_group(flat.shape, rank) == 0, flat, 0.0)
    total = jnp.zeros((shards * step, lanes), f32)
    tokens = tokens_ref[...].reshape(shards, 4, step, -1)
    for i in range(4):
        at = pltpu.roll(p, i * rank, 1) if i else p
        high = at.astype(bf16)
        low = (at - high.astype(f32)).astype(bf16)
        part = tokens[:, i].reshape(shards * step, -1)
        total = total + dot(part, high, ((1,), (0,))) + dot(part, low, ((1,), (0,)))
    out_ref[:, :own] = jnp.broadcast_to(sums[None], (shards, own, lanes))
    out_ref[:, own:] = total.reshape(shards, step, lanes)


def key_products(
    at_ref, tokens_ref, base_ref, momentum_ref, sa_ref, ka_ref, sb_ref, kb_ref
):
    xl, y0 = at_ref[0], at_ref[1]
    block, half = sa_ref.shape[1:]
    settled = base_ref[...].astype(f32) - own_mom * momentum_ref[...].astype(f32)
    settled = settled.astype(bf16)
    left, right = settled[:, :half], settled[:, half:]

    def rows(i):
        return tokens_ref[pl.ds(pl.multiple_of(i * block, block), block)]

    for j in range(sa_ref.shape[0]):
        sa_ref[j] = dot(rows(2 * j + 1 - xl), left, ((1,), (0,))).astype(bf16)
        sb_ref[j] = dot(
            rows((j // 2) * 4 + (1 - y0) * 2 + j % 2), right, ((1,), (0,))
        ).astype(bf16)
    for j in range(sa_ref.shape[0]):
        ka_ref[j] = dot(rows(2 * j + xl), left, ((1,), (0,)))
        kb_ref[j] = dot(rows((j // 2) * 4 + y0 * 2 + j % 2), right, ((1,), (0,)))


def in_vmem(kernel, out_shape, n, scalars=0, **cost):
    whole = pl.BlockSpec(memory_space=pltpu.VMEM)
    small = pl.BlockSpec(memory_space=pltpu.SMEM)
    return pl.pallas_call(
        kernel,
        out_shape=out_shape,
        in_specs=[small] * scalars + [whole] * (n - scalars),
        out_specs=jax.tree.map(lambda _: whole, out_shape),
        cost_estimate=pl.CostEstimate(**cost),
    )


def on_device(local_weights, outer_base, momentum, error_feedback, q_start, tokens):
    replicas, shards = lax.axis_size(peers), lax.axis_size(shard)
    rows, kv = outer_base.shape
    rank = q_start.shape[1]
    own = rows // replicas
    cols = kv // replicas
    core = lax.axis_index("core")
    base = outer_base.astype(f32)
    own_tokens = tokens[0]
    block = own_tokens.shape[0] // shards
    shape = jax.ShapeDtypeStruct

    pseudo = base - local_weights[0].astype(f32) + error_feedback[0].astype(f32)
    halves = pseudo.reshape(2, rows // 2, kv)
    pair = pick(halves, core, 0) + swap(pick(halves, 1 - core, 0), "core")
    first = exchange(
        jnp.concatenate(
            [
                pair.astype(bf16).reshape(replicas // 2, own, kv),
                jnp.broadcast_to(momentum.T, (replicas // 2, cols, rows)),
            ],
            axis=1,
        ),
        chips,
    )
    second = in_vmem(
        functools.partial(moments, own=own, rank=rank, replicas=replicas),
        shape((replicas, own, 4 * rank), f32),
        2,
        flops=20000000,
        bytes_accessed=1000000,
        transcendentals=0,
    )(first, jnp.tile(q_start, (1, 4)))
    second = exchange(second, peers)

    my_momentum = first[:, own:]
    its_momentum = swap(my_momentum, "core")
    full_momentum = jnp.stack(
        [
            jnp.where(core == 0, my_momentum, its_momentum),
            jnp.where(core == 0, its_momentum, my_momentum),
        ],
        axis=1,
    ).reshape(kv, rows)
    full_momentum = full_momentum.T

    part = (shards // 2, block, kv // 2)
    send_a, keep_a, send_b, keep_b = in_vmem(
        key_products,
        (shape(part, bf16), shape(part, f32), shape(part, bf16), shape(part, f32)),
        4,
        1,
        flops=2 * 2048 * 512 * 512,
        bytes_accessed=9000000,
        transcendentals=0,
    )(
        jnp.stack([lax.axis_index("xl"), lax.axis_index("y0")]).astype(jnp.int32),
        own_tokens,
        outer_base,
        full_momentum,
    )
    key_a = keep_a + swap(send_a, "xl").astype(f32)
    key_b = keep_b + swap(send_b, "y0").astype(f32)
    quarter = (shards // 4, 2, block, kv // 2)
    key_a = halve(key_a.reshape(quarter), "y0", 1)
    key_b = halve(key_b.reshape(quarter), "xl", 1)
    key_part = jnp.concatenate([key_a, key_b], axis=-1)
    place = lax.axis_index(("y2", "y1"))
    key_sum = pick(key_part, place, 0)
    for d in (1, 2, 3):
        away = pick(key_part, place ^ d, 0).astype(bf16)
        key_sum = key_sum + lax.ppermute(
            away, ("y2", "y1"), [(i, i ^ d) for i in range(4)]
        ).astype(f32)

    third = in_vmem(
        functools.partial(token_products, own=own, rank=rank),
        shape((shards, own + block // 4, 4 * rank), f32),
        2,
        flops=500000000,
        bytes_accessed=3000000,
        transcendentals=0,
    )(second, own_tokens)
    third = jnp.sum(exchange(third, shard), axis=0)
    sums, token_sum = third[:own], third[own:]
    fourth = copy_for_each(sums, peers)

    token_sum = jnp.concatenate(
        [token_sum[:, i * rank : (i + 1) * rank] for i in range(4)], axis=0
    )
    gram = jnp.concatenate([sums[:, rank : 2 * rank], sums[:, 2 * rank : 3 * rank]], axis=0)
    p_mean = second[:, :, :rank].reshape(rows, rank)
    factor_low = jnp.linalg.cholesky(gram)
    inverse = jax.scipy.linalg.solve_triangular(
        factor_low, jnp.eye(rank, dtype=f32), lower=True
    )
    basis = jnp.dot(p_mean, inverse.T, precision=highest)
    token_basis = jnp.dot(token_sum, inverse.T, precision=highest)

    q_sum = fourth[:, :, 3 * rank :].reshape(kv, rank)
    q_mean = jnp.dot(q_sum, inverse.T, precision=highest)
    update = jnp.dot(basis, q_mean.T, precision=highest)
    new_error = (pseudo - update).astype(bf16)[None]
    moment = outer_mu * full_momentum.astype(f32) + update
    new_base = (base - outer_rate * (outer_mu * moment + update)).astype(bf16)
    at = lax.axis_index(chips + ("core",)) * cols
    own_q = lax.dynamic_slice_in_dim(q_mean, at, cols, 0)
    new_momentum = outer_mu * momentum.astype(f32) + jnp.dot(
        basis, own_q.T, precision=highest
    )
    key_rows = key_sum - own_upd * jnp.dot(token_basis, q_mean.T, precision=highest)
    return (
        new_base,
        new_momentum.astype(bf16),
        new_error,
        key_rows.astype(bf16)[None],
    )


def solution(mesh):
    fine = Mesh(
        mesh.devices.reshape(8, 2, 2, 2, 2, 2, 2), chips + ("core",) + shard
    )
    replica = chips + ("core",)
    in_specs = (
        P(replica, shard, None),
        P(shard, None),
        P(shard, replica),
        P(replica, shard, None),
        P(),
        P(replica, None, shard),
    )
    out_specs = (
        P(shard, None),
        P(shard, replica),
        P(replica, shard, None),
        P(replica, shard, None),
    )
    return jax.shard_map(
        on_device, mesh=fine, in_specs=in_specs, out_specs=out_specs, check_vma=False
    )
```

```python
import functools

import jax
import jax.numpy as jnp
from jax import lax
from jax.experimental import pallas as pl
from jax.experimental.pallas import tpu as pltpu
from jax.sharding import Mesh, PartitionSpec as P


outer_mu = 0.9
outer_rate = 0.7
own_mom = outer_rate * outer_mu * outer_mu
own_upd = outer_rate * (outer_mu + 1.0)


chips = ("z", "xh")
peers = ("core", "z", "xh")
shard = ("y2", "y1", "y0", "xl")
f32, bf16 = jnp.float32, jnp.bfloat16
highest = lax.Precision.HIGHEST


def swap(x, axis):
    return lax.ppermute(x, axis, [(0, 1), (1, 0)])


def exchange(x, axis):
    return lax.all_to_all(x, axis, 0, 0, tiled=True)


def copy_for_each(x, axis):
    return exchange(jnp.broadcast_to(x, (lax.axis_size(axis), *x.shape)), axis)


def pick(x, at, dim):
    return lax.dynamic_index_in_dim(x, at, dim, keepdims=False)


def halve(x, axis, dim):
    me = lax.axis_index(axis)
    other = swap(pick(x, 1 - me, dim).astype(bf16), axis)
    return pick(x, me, dim) + other.astype(f32)


def dot(a, b, dims, precision=None):
    return lax.dot_general(
        a, b, (dims, ((), ())), precision=precision, preferred_element_type=f32
    )


def lane_group(shape, rank):
    return lax.broadcasted_iota(jnp.int32, shape, 1) // rank


def moments(first_ref, q_ref, out_ref, *, own, rank, replicas):
    mean = jnp.sum(first_ref[...].astype(f32), axis=0) * (1.0 / replicas)
    q = jnp.concatenate([q_ref[...]] * 4, axis=0)
    p = dot(mean, q, ((1,), (1,)), highest)
    group = lane_group(p.shape, rank)
    p_at = [jnp.where(group == i, p, 0.0) for i in range(4)]
    upper = dot(p_at[0], p_at[1], ((0,), (0,)), highest)
    lower = dot(p_at[0], p_at[2], ((0,), (0,)), highest)
    same = p_at[0] + upper[:own] + lower[own : 2 * own]
    q_rows = dot(mean, p_at[3], ((0,), (0,)), highest)
    out_ref[...] = q_rows.reshape(out_ref.shape) + same[None]


def token_products(second_ref, tokens_ref, out_ref, *, own, rank):
    peers_, rows_, lanes = second_ref.shape
    shards = out_ref.shape[0]
    block = tokens_ref.shape[0] // shards
    step = block // 4
    second = second_ref[...]
    sums = jnp.sum(second, axis=0)
    flat = second.reshape(peers_ * rows_, lanes)
    p = jnp.where(lane_group(flat.shape, rank) == 0, flat, 0.0)
    total = jnp.zeros((shards * step, lanes), f32)
    tokens = tokens_ref[...].reshape(shards, 4, step, -1)
    for i in range(4):
        at = pltpu.roll(p, i * rank, 1) if i else p
        high = at.astype(bf16)
        low = (at - high.astype(f32)).astype(bf16)
        part = tokens[:, i].reshape(shards * step, -1)
        total = total + dot(part, high, ((1,), (0,))) + dot(part, low, ((1,), (0,)))
    out_ref[:, :own] = jnp.broadcast_to(sums[None], (shards, own, lanes))
    out_ref[:, own:] = total.reshape(shards, step, lanes)


def key_products(tokens_ref, base_ref, momentum_ref, sa_ref, ka_ref, sb_ref, kb_ref):
    xl, y0 = lax.axis_index("xl"), lax.axis_index("y0")
    block, half = sa_ref.shape[1:]
    settled = base_ref[...].astype(f32) - own_mom * momentum_ref[...].astype(f32)
    settled = settled.astype(bf16)
    left, right = settled[:, :half], settled[:, half:]

    def rows(i):
        return tokens_ref[pl.ds(pl.multiple_of(i * block, block), block)]

    for j in range(sa_ref.shape[0]):
        sa_ref[j] = dot(rows(2 * j + 1 - xl), left, ((1,), (0,))).astype(bf16)
        sb_ref[j] = dot(
            rows((j // 2) * 4 + (1 - y0) * 2 + j % 2), right, ((1,), (0,))
        ).astype(bf16)
    for j in range(sa_ref.shape[0]):
        ka_ref[j] = dot(rows(2 * j + xl), left, ((1,), (0,)))
        kb_ref[j] = dot(rows((j // 2) * 4 + y0 * 2 + j % 2), right, ((1,), (0,)))


def in_vmem(kernel, out_shape, n, mib, flops):
    whole = pl.BlockSpec(memory_space=pltpu.VMEM)
    return pl.pallas_call(
        kernel,
        out_shape=out_shape,
        in_specs=[whole] * n,
        out_specs=jax.tree.map(lambda _: whole, out_shape),
        cost_estimate=pl.CostEstimate(
            flops=flops, bytes_accessed=flops // 100, transcendentals=0
        ),
        compiler_params=pltpu.CompilerParams(vmem_limit_bytes=mib << 20) if mib else None,
    )


def on_device(local_weights, outer_base, momentum, error_feedback, q_start, tokens):
    replicas, shards = lax.axis_size(peers), lax.axis_size(shard)
    rows, kv = outer_base.shape
    rank = q_start.shape[1]
    own = rows // replicas
    cols = kv // replicas
    core = lax.axis_index("core")
    base = outer_base.astype(f32)
    own_tokens = tokens[0]
    block = own_tokens.shape[0] // shards
    shape = jax.ShapeDtypeStruct

    my_momentum = copy_for_each(momentum.T, chips)

    pseudo = base - local_weights[0].astype(f32) + error_feedback[0].astype(f32)
    halves = pseudo.reshape(2, rows // 2, kv)
    pair = swap(pick(halves, 1 - core, 0), "core")
    pair = (pick(halves, core, 0) + pair).astype(bf16)
    pair, my_momentum = lax.optimization_barrier((pair, my_momentum))
    first = exchange(pair.reshape(replicas // 2, own, kv), chips)
    second = in_vmem(
        functools.partial(moments, own=own, rank=rank, replicas=replicas),
        shape((replicas, own, 4 * rank), f32),
        2,
        0,
        40000000,
    )(first, q_start.T)
    second = exchange(second, peers)

    its_momentum = swap(my_momentum, "core")
    full_momentum = jnp.stack(
        [
            jnp.where(core == 0, my_momentum, its_momentum),
            jnp.where(core == 0, its_momentum, my_momentum),
        ],
        axis=1,
    ).reshape(kv, rows)
    full_momentum = full_momentum.T

    part = (shards // 2, block, kv // 2)
    send_a, keep_a, send_b, keep_b = in_vmem(
        key_products,
        (shape(part, bf16), shape(part, f32), shape(part, bf16), shape(part, f32)),
        3,
        0,
        2 * tokens.shape[1] * rows * kv,
    )(own_tokens, outer_base, full_momentum)
    key_a = swap(send_a, "xl")
    key_b = swap(send_b, "y0")
    key_a = keep_a + key_a.astype(f32)
    key_b = keep_b + key_b.astype(f32)
    quarter = (shards // 4, 2, block, kv // 2)
    key_a = halve(key_a.reshape(quarter), "y0", 1)
    key_b = halve(key_b.reshape(quarter), "xl", 1)
    key_part = jnp.concatenate([key_a, key_b], axis=-1)
    place = lax.axis_index(("y2", "y1"))
    key_sum = pick(key_part, place, 0)
    for d in (1, 2, 3):
        away = pick(key_part, place ^ d, 0).astype(bf16)
        away = lax.ppermute(away, ("y2", "y1"), [(i, i ^ d) for i in range(4)])
        key_sum = key_sum + away.astype(f32)

    third = in_vmem(
        functools.partial(token_products, own=own, rank=rank),
        shape((shards, own + block // 4, 4 * rank), f32),
        2,
        0,
        500000000,
    )(second, own_tokens)
    third = exchange(third, shard)
    third = jnp.sum(third, axis=0)
    sums, token_sum = third[:own], third[own:]
    fourth = copy_for_each(sums, peers)

    token_sum = jnp.concatenate(
        [token_sum[:, i * rank : (i + 1) * rank] for i in range(4)], axis=0
    )
    gram = jnp.concatenate([sums[:, rank : 2 * rank], sums[:, 2 * rank : 3 * rank]], axis=0)
    p_mean = second[:, :, :rank].reshape(rows, rank)
    factor_low = jnp.linalg.cholesky(gram)
    inverse = jax.scipy.linalg.solve_triangular(
        factor_low, jnp.eye(rank, dtype=f32), lower=True
    )
    basis = jnp.dot(p_mean, inverse.T, precision=highest)
    token_basis = jnp.dot(token_sum, inverse.T, precision=highest)

    q_sum = fourth[:, :, 3 * rank :].reshape(kv, rank)
    q_mean = jnp.dot(q_sum, inverse.T, precision=highest)
    update = jnp.dot(basis, q_mean.T, precision=highest)
    new_error = (pseudo - update).astype(bf16)[None]
    moment = outer_mu * full_momentum.astype(f32) + update
    new_base = (base - outer_rate * (outer_mu * moment + update)).astype(bf16)
    at = lax.axis_index(chips + ("core",)) * cols
    own_q = lax.dynamic_slice_in_dim(q_mean, at, cols, 0)
    new_momentum = outer_mu * momentum.astype(f32) + jnp.dot(
        basis, own_q.T, precision=highest
    )
    key_rows = key_sum - own_upd * jnp.dot(token_basis, q_mean.T, precision=highest)
    return (
        new_base,
        new_momentum.astype(bf16),
        new_error,
        key_rows.astype(bf16)[None],
    )


def solution(mesh):
    fine = Mesh(
        mesh.devices.reshape(8, 2, 2, 2, 2, 2, 2), chips + ("core",) + shard
    )
    replica = chips + ("core",)
    in_specs = (
        P(replica, shard, None),
        P(shard, None),
        P(shard, replica),
        P(replica, shard, None),
        P(),
        P(replica, None, shard),
    )
    out_specs = (
        P(shard, None),
        P(shard, replica),
        P(replica, shard, None),
        P(replica, shard, None),
    )

    def step(*arrays):
        return on_device(*arrays)

    step = jax.shard_map(
        step, mesh=fine, in_specs=in_specs, out_specs=out_specs, check_vma=False
    )
    return step
```

```python
import functools

import jax
import jax.numpy as jnp
from jax import lax
from jax.experimental import pallas as pl
from jax.experimental.pallas import tpu as pltpu
from jax.sharding import Mesh, PartitionSpec as P


outer_mu = 0.9
outer_rate = 0.7
own_mom = outer_rate * outer_mu * outer_mu
own_upd = outer_rate * (outer_mu + 1.0)


chips = ("z", "xh")
peers = ("core", "z", "xh")
shard = ("y2", "y1", "y0", "xl")
f32, bf16 = jnp.float32, jnp.bfloat16
highest = lax.Precision.HIGHEST


def swap(x, axis):
    return lax.ppermute(x, axis, [(0, 1), (1, 0)])


def exchange(x, axis):
    return lax.all_to_all(x, axis, 0, 0, tiled=True)


def copy_for_each(x, axis):
    return exchange(jnp.broadcast_to(x, (lax.axis_size(axis), *x.shape)), axis)


def pick(x, at, dim):
    return lax.dynamic_index_in_dim(x, at, dim, keepdims=False)


def halve(x, axis, dim):
    me = lax.axis_index(axis)
    other = swap(pick(x, 1 - me, dim).astype(bf16), axis)
    return pick(x, me, dim) + other.astype(f32)


def dot(a, b, dims, precision=None):
    return lax.dot_general(
        a, b, (dims, ((), ())), precision=precision, preferred_element_type=f32
    )


def lane_group(shape, rank):
    return lax.broadcasted_iota(jnp.int32, shape, 1) // rank


def moments(first_ref, q_ref, out_ref, *, own, rank, replicas):
    mean = jnp.sum(first_ref[...].astype(f32), axis=0) * (1.0 / replicas)
    q = jnp.concatenate([q_ref[...]] * 4, axis=0)
    p = dot(mean, q, ((1,), (1,)), highest)
    group = lane_group(p.shape, rank)
    p_at = [jnp.where(group == i, p, 0.0) for i in range(4)]
    upper = dot(p_at[0], p_at[1], ((0,), (0,)), highest)
    lower = dot(p_at[0], p_at[2], ((0,), (0,)), highest)
    same = p_at[0] + upper[:own] + lower[own : 2 * own]
    q_rows = dot(mean, p_at[3], ((0,), (0,)), highest)
    out_ref[...] = q_rows.reshape(out_ref.shape) + same[None]


def token_products(second_ref, tokens_ref, out_ref, *, own, rank):
    peers_, rows_, lanes = second_ref.shape
    shards = out_ref.shape[0]
    block = tokens_ref.shape[0] // shards
    step = block // 4
    second = second_ref[...]
    sums = jnp.sum(second, axis=0)
    flat = second.reshape(peers_ * rows_, lanes)
    p = jnp.where(lane_group(flat.shape, rank) == 0, flat, 0.0)
    total = jnp.zeros((shards * step, lanes), f32)
    tokens = tokens_ref[...].reshape(shards, 4, step, -1)
    for i in range(4):
        at = pltpu.roll(p, i * rank, 1) if i else p
        high = at.astype(bf16)
        low = (at - high.astype(f32)).astype(bf16)
        part = tokens[:, i].reshape(shards * step, -1)
        total = total + dot(part, high, ((1,), (0,))) + dot(part, low, ((1,), (0,)))
    out_ref[:, :own] = jnp.broadcast_to(sums[None], (shards, own, lanes))
    out_ref[:, own:] = total.reshape(shards, step, lanes)


def key_products(tokens_ref, base_ref, momentum_ref, sa_ref, ka_ref, sb_ref, kb_ref):
    xl, y0 = lax.axis_index("xl"), lax.axis_index("y0")
    block, half = sa_ref.shape[1:]
    settled = base_ref[...].astype(f32) - own_mom * momentum_ref[...].astype(f32)
    settled = settled.astype(bf16)
    left, right = settled[:, :half], settled[:, half:]

    def rows(i):
        return tokens_ref[pl.ds(pl.multiple_of(i * block, block), block)]

    for j in range(sa_ref.shape[0]):
        sa_ref[j] = dot(rows(2 * j + 1 - xl), left, ((1,), (0,))).astype(bf16)
        sb_ref[j] = dot(
            rows((j // 2) * 4 + (1 - y0) * 2 + j % 2), right, ((1,), (0,))
        ).astype(bf16)
    for j in range(sa_ref.shape[0]):
        ka_ref[j] = dot(rows(2 * j + xl), left, ((1,), (0,)))
        kb_ref[j] = dot(rows((j // 2) * 4 + y0 * 2 + j % 2), right, ((1,), (0,)))


def shard_sums(third_ref, copies_ref, total_ref):
    total = jnp.sum(third_ref[...], axis=0)
    total_ref[...] = total
    copies_ref[...] = jnp.broadcast_to(
        total[None, : copies_ref.shape[1]], copies_ref.shape
    )


def bases(total_ref, second_ref, basis_ref, token_ref, inverse_ref, *, own, rank):
    total = total_ref[...]
    lanes = total.shape[1]
    sums, token_sum = total[:own], total[own:]
    left = jnp.concatenate(
        [pltpu.roll(sums, lanes - rank, 1), pltpu.roll(sums, lanes - 2 * rank, 1)], axis=0
    )
    row = lax.broadcasted_iota(jnp.int32, (rank, lanes), 0)
    lane = lax.broadcasted_iota(jnp.int32, (rank, lanes), 1)
    work = jnp.where(lane < rank, left, jnp.where(lane == row + rank, 1.0, 0.0))
    for j in range(rank - 1):
        ratio = work[:, j : j + 1] / work[j : j + 1, j : j + 1]
        work = work - jnp.where(row > j, ratio * work[j : j + 1], 0.0)
    pivot = jnp.sum(jnp.where(lane == row, work, 0.0), axis=1, keepdims=True)
    work = jnp.where((lane >= rank) & (lane < 2 * rank), work / jnp.sqrt(pivot), 0.0)
    rest = jnp.zeros((lanes - rank, lanes), f32)
    at = [
        jnp.concatenate([pltpu.roll(work, ((i - 1) * rank) % lanes, 1), rest], axis=0)
        for i in (0, 2, 3)
    ]
    at.insert(1, jnp.concatenate([work, rest], axis=0))
    flat = second_ref[...].reshape(-1, lanes)
    basis_ref[...] = dot(flat, at[0], ((1,), (1,)), highest)
    token_ref[...] = jnp.concatenate(
        [dot(token_sum, a, ((1,), (1,)), highest) for a in at], axis=0
    )
    inverse_ref[...] = at[3]


def outputs(
    fourth_ref, inverse_ref, basis_ref, token_ref, local_ref, base_ref, error_ref,
    full_ref, momentum_ref, base_out, momentum_out, error_out, key_out, q_scratch,
):
    last = ((1,), (1,))
    rows_, cols = base_ref.shape[0], momentum_ref.shape[0]
    flat = fourth_ref[...].reshape(-1, fourth_ref.shape[2])
    q = dot(flat, inverse_ref[...], last, highest)
    q_scratch[...] = q
    key_out[...] = own_upd * dot(token_ref[...], q, last, highest)
    at = lax.axis_index(chips + ("core",)) * cols
    own_q = q_scratch[pl.ds(pl.multiple_of(at, cols), cols)]
    momentum_out[...] = (
        outer_mu * momentum_ref[...].astype(f32)
        + dot(own_q, basis_ref[...], last, highest)
    ).astype(bf16)
    step = rows_ // 4
    for i in range(4):
        here = slice(i * step, (i + 1) * step)
        update = dot(basis_ref[here], q, last, highest)
        base = base_ref[here].astype(f32)
        pseudo = base - local_ref[here].astype(f32) + error_ref[here].astype(f32)
        error_out[here] = (pseudo - update).astype(bf16)
        moment = outer_mu * full_ref[here].astype(f32) + update
        base_out[here] = (base - outer_rate * (outer_mu * moment + update)).astype(bf16)


def in_vmem(kernel, out_shape, n, mib, flops, scratch=()):
    whole = pl.BlockSpec(memory_space=pltpu.VMEM)
    return pl.pallas_call(
        kernel,
        out_shape=out_shape,
        in_specs=[whole] * n,
        out_specs=jax.tree.map(lambda _: whole, out_shape),
        scratch_shapes=scratch,
        cost_estimate=pl.CostEstimate(
            flops=flops, bytes_accessed=flops // 100, transcendentals=0
        ),
        compiler_params=pltpu.CompilerParams(vmem_limit_bytes=mib << 20) if mib else None,
    )


def on_device(local_weights, outer_base, momentum, error_feedback, q_start, tokens):
    replicas, shards = lax.axis_size(peers), lax.axis_size(shard)
    rows, kv = outer_base.shape
    rank = q_start.shape[1]
    own = rows // replicas
    cols = kv // replicas
    core = lax.axis_index("core")
    base = outer_base.astype(f32)
    own_tokens = tokens[0]
    block = own_tokens.shape[0] // shards
    shape = jax.ShapeDtypeStruct

    my_momentum = copy_for_each(momentum.T, chips)

    pseudo = base - local_weights[0].astype(f32) + error_feedback[0].astype(f32)
    halves = pseudo.reshape(2, rows // 2, kv)
    pair = swap(pick(halves, 1 - core, 0), "core")
    pair = (pick(halves, core, 0) + pair).astype(bf16)
    pair, my_momentum = lax.optimization_barrier((pair, my_momentum))
    first = exchange(pair.reshape(replicas // 2, own, kv), chips)
    second = in_vmem(
        functools.partial(moments, own=own, rank=rank, replicas=replicas),
        shape((replicas, own, 4 * rank), f32),
        2,
        0,
        40000000,
    )(first, q_start.T)
    second = exchange(second, peers)

    its_momentum = swap(my_momentum, "core")
    full_momentum = jnp.stack(
        [
            jnp.where(core == 0, my_momentum, its_momentum),
            jnp.where(core == 0, its_momentum, my_momentum),
        ],
        axis=1,
    ).reshape(kv, rows)
    full_momentum = full_momentum.T

    part = (shards // 2, block, kv // 2)
    send_a, keep_a, send_b, keep_b = in_vmem(
        key_products,
        (shape(part, bf16), shape(part, f32), shape(part, bf16), shape(part, f32)),
        3,
        0,
        2 * tokens.shape[1] * rows * kv,
    )(own_tokens, outer_base, full_momentum)
    key_a = swap(send_a, "xl")
    key_b = swap(send_b, "y0")
    key_a = keep_a + key_a.astype(f32)
    key_b = keep_b + key_b.astype(f32)
    quarter = (shards // 4, 2, block, kv // 2)
    key_a = halve(key_a.reshape(quarter), "y0", 1)
    key_b = halve(key_b.reshape(quarter), "xl", 1)
    key_part = jnp.concatenate([key_a, key_b], axis=-1).reshape(2, 2, block, kv)
    key_part = halve(key_part, "y1", 1)
    key_sum = halve(key_part, "y2", 0)

    third = in_vmem(
        functools.partial(token_products, own=own, rank=rank),
        shape((shards, own + block // 4, 4 * rank), f32),
        2,
        0,
        500000000,
    )(second, own_tokens)
    third = exchange(third, shard)
    lanes = 4 * rank
    copies, total = in_vmem(
        shard_sums,
        (shape((replicas, own, lanes), f32), shape(third.shape[1:], f32)),
        1,
        0,
        1000000,
    )(third)
    fourth = exchange(copies, peers)
    basis, token_basis, inverse = in_vmem(
        functools.partial(bases, own=own, rank=rank),
        (
            shape((rows, lanes), f32),
            shape((block, lanes), f32),
            shape((lanes, lanes), f32),
        ),
        2,
        0,
        100000000,
    )(total, second)
    new_base, new_momentum, new_error, key_low = in_vmem(
        outputs,
        (
            shape((rows, kv), bf16),
            shape((cols, rows), bf16),
            shape((rows, kv), bf16),
            shape((block, kv), f32),
        ),
        9,
        0,
        400000000,
        (pltpu.VMEM((kv, lanes), f32),),
    )(
        fourth,
        inverse,
        basis,
        token_basis,
        local_weights[0],
        outer_base,
        error_feedback[0],
        full_momentum,
        momentum.T,
    )
    key_rows = (key_sum - key_low).astype(bf16)
    return new_base, new_momentum.T, new_error[None], key_rows[None]


def solution(mesh):
    fine = Mesh(
        mesh.devices.reshape(8, 2, 2, 2, 2, 2, 2), chips + ("core",) + shard
    )
    replica = chips + ("core",)
    in_specs = (
        P(replica, shard, None),
        P(shard, None),
        P(shard, replica),
        P(replica, shard, None),
        P(),
        P(replica, None, shard),
    )
    out_specs = (
        P(shard, None),
        P(shard, replica),
        P(replica, shard, None),
        P(replica, shard, None),
    )

    def step(*arrays):
        return on_device(*arrays)

    step = jax.shard_map(
        step, mesh=fine, in_specs=in_specs, out_specs=out_specs, check_vma=False
    )
    return step
```

```python
import functools

import jax
import jax.numpy as jnp
from jax import lax
from jax.experimental import pallas as pl
from jax.experimental.pallas import tpu as pltpu
from jax.sharding import Mesh, PartitionSpec as P


outer_mu = 0.9
outer_rate = 0.7
own_mom = outer_rate * outer_mu * outer_mu
own_upd = outer_rate * (outer_mu + 1.0)


chips = ("z", "xh")
peers = ("core", "z", "xh")
shard = ("y2", "y1", "y0", "xl")
f32, bf16 = jnp.float32, jnp.bfloat16
highest = lax.Precision.HIGHEST


def swap(x, axis):
    return lax.ppermute(x, axis, [(0, 1), (1, 0)])


def exchange(x, axis):
    return lax.all_to_all(x, axis, 0, 0, tiled=True)


def copy_for_each(x, axis):
    return exchange(jnp.broadcast_to(x, (lax.axis_size(axis), *x.shape)), axis)


def pick(x, at, dim):
    return lax.dynamic_index_in_dim(x, at, dim, keepdims=False)


def halve(x, axis, dim):
    me = lax.axis_index(axis)
    other = swap(pick(x, 1 - me, dim).astype(bf16), axis)
    return pick(x, me, dim) + other.astype(f32)


def dot(a, b, dims, precision=None):
    return lax.dot_general(
        a, b, (dims, ((), ())), precision=precision, preferred_element_type=f32
    )


def lane_group(shape, rank):
    return lax.broadcasted_iota(jnp.int32, shape, 1) // rank


def moments(first_ref, q_ref, hbm_ref, out_ref, *, own, rank, replicas):
    mean = jnp.sum(first_ref[...].astype(f32), axis=0) * (1.0 / replicas)
    q = jnp.concatenate([q_ref[...]] * 4, axis=0)
    p = dot(mean, q, ((1,), (1,)), highest)
    group = lane_group(p.shape, rank)
    p_at = [jnp.where(group == i, p, 0.0) for i in range(4)]
    upper = dot(p_at[0], p_at[1], ((0,), (0,)), highest)
    lower = dot(p_at[0], p_at[2], ((0,), (0,)), highest)
    same = p_at[0] + upper[:own] + lower[own : 2 * own]
    q_rows = dot(mean, p_at[3], ((0,), (0,)), highest)
    out_ref[...] = q_rows.reshape(out_ref.shape) + same[None]
    pltpu.sync_copy(out_ref, hbm_ref)


def token_products(second_ref, tokens_ref, hbm_ref, out_ref, *, own, rank):
    peers_, rows_, lanes = second_ref.shape
    shards = out_ref.shape[0]
    block = tokens_ref.shape[0] // shards
    step = block // 4
    second = second_ref[...]
    sums = jnp.sum(second, axis=0)
    flat = second.reshape(peers_ * rows_, lanes)
    p = jnp.where(lane_group(flat.shape, rank) == 0, flat, 0.0)
    total = jnp.zeros((shards * step, lanes), f32)
    tokens = tokens_ref[...].reshape(shards, 4, step, -1)
    for i in range(4):
        at = pltpu.roll(p, i * rank, 1) if i else p
        high = at.astype(bf16)
        low = (at - high.astype(f32)).astype(bf16)
        part = tokens[:, i].reshape(shards * step, -1)
        total = total + dot(part, high, ((1,), (0,))) + dot(part, low, ((1,), (0,)))
    out_ref[:, :own] = jnp.broadcast_to(sums[None], (shards, own, lanes))
    out_ref[:, own:] = total.reshape(shards, step, lanes)
    pltpu.sync_copy(out_ref, hbm_ref)


def key_products(
    tokens_ref, base_ref, momentum_ref, left_ref, right_ref, keep_ref, sent, sems
):
    y0 = lax.axis_index("y0")
    settled = base_ref[...].astype(f32) - own_mom * momentum_ref[...].astype(f32)
    settled = settled.astype(bf16)
    groups, block, cols = keep_ref.shape[0] // 2, keep_ref.shape[1], keep_ref.shape[2]
    half = cols // 2

    def product(i, parity):
        at = pl.multiple_of((2 * i + parity) * 2 * block, 2 * block)
        part = dot(tokens_ref[pl.ds(at, 2 * block)], settled, ((1,), (0,)))
        return part.reshape(2, block, cols)

    for i in range(groups):
        sent[2 * i : 2 * i + 2] = product(i, 1 - y0).astype(bf16)
    copies = [
        pltpu.make_async_copy(sent.at[:, :, :half], left_ref, sems.at[0]),
        pltpu.make_async_copy(sent.at[:, :, half:], right_ref, sems.at[1]),
    ]
    for copy in copies:
        copy.start()
    for i in range(groups):
        keep_ref[2 * i : 2 * i + 2] = product(i, y0)
    for copy in copies:
        copy.wait()


def shard_sums(third_ref, hbm_ref, total_ref, copies_ref):
    total = jnp.sum(third_ref[...], axis=0)
    total_ref[...] = total
    copies_ref[...] = jnp.broadcast_to(
        total[None, : copies_ref.shape[1]], copies_ref.shape
    )
    pltpu.sync_copy(copies_ref, hbm_ref)


def bases(total_ref, second_ref, basis_ref, token_ref, inverse_ref, *, own, rank):
    total = total_ref[...]
    lanes = total.shape[1]
    sums, token_sum = total[:own], total[own:]
    left = jnp.concatenate(
        [pltpu.roll(sums, lanes - rank, 1), pltpu.roll(sums, lanes - 2 * rank, 1)], axis=0
    )
    row = lax.broadcasted_iota(jnp.int32, (rank, lanes), 0)
    lane = lax.broadcasted_iota(jnp.int32, (rank, lanes), 1)
    work = jnp.where(lane < rank, left, jnp.where(lane == row + rank, 1.0, 0.0))
    for j in range(rank - 1):
        ratio = work[:, j : j + 1] / work[j : j + 1, j : j + 1]
        work = work - jnp.where(row > j, ratio * work[j : j + 1], 0.0)
    pivot = jnp.sum(jnp.where(lane == row, work, 0.0), axis=1, keepdims=True)
    work = jnp.where((lane >= rank) & (lane < 2 * rank), work / jnp.sqrt(pivot), 0.0)
    rest = jnp.zeros((lanes - rank, lanes), f32)
    at = [
        jnp.concatenate([pltpu.roll(work, ((i - 1) * rank) % lanes, 1), rest], axis=0)
        for i in (0, 2, 3)
    ]
    at.insert(1, jnp.concatenate([work, rest], axis=0))
    flat = second_ref[...].reshape(-1, lanes)
    basis_ref[...] = dot(flat, at[0], ((1,), (1,)), highest)
    token_ref[...] = jnp.concatenate(
        [dot(token_sum, a, ((1,), (1,)), highest) for a in at], axis=0
    )
    inverse_ref[...] = at[3]


def outputs(
    fourth_ref, inverse_ref, basis_ref, token_ref, local_ref, base_ref, error_ref,
    full_ref, momentum_ref, base_out, momentum_out, error_out, key_out, q_scratch,
):
    last = ((1,), (1,))
    rows_, cols = base_ref.shape[0], momentum_ref.shape[0]
    flat = fourth_ref[...].reshape(-1, fourth_ref.shape[2])
    q = dot(flat, inverse_ref[...], last, highest)
    q_scratch[...] = q
    key_out[...] = own_upd * dot(token_ref[...], q, last, highest)
    at = lax.axis_index(chips + ("core",)) * cols
    own_q = q_scratch[pl.ds(pl.multiple_of(at, cols), cols)]
    momentum_out[...] = (
        outer_mu * momentum_ref[...].astype(f32)
        + dot(own_q, basis_ref[...], last, highest)
    ).astype(bf16)
    step = rows_ // 4
    for i in range(4):
        here = slice(i * step, (i + 1) * step)
        update = dot(basis_ref[here], q, last, highest)
        base = base_ref[here].astype(f32)
        pseudo = base - local_ref[here].astype(f32) + error_ref[here].astype(f32)
        error_out[here] = (pseudo - update).astype(bf16)
        moment = outer_mu * full_ref[here].astype(f32) + update
        base_out[here] = (base - outer_rate * (outer_mu * moment + update)).astype(bf16)


def in_vmem(kernel, out_shape, n, mib, flops, scratch=(), far=0):
    whole = pl.BlockSpec(memory_space=pltpu.VMEM)
    hbm = pl.BlockSpec(memory_space=pltpu.HBM)
    return pl.pallas_call(
        kernel,
        out_shape=out_shape,
        in_specs=[whole] * n,
        out_specs=tuple(hbm if i < far else whole for i in range(len(out_shape))),
        scratch_shapes=scratch,
        cost_estimate=pl.CostEstimate(
            flops=flops, bytes_accessed=flops // 100, transcendentals=0
        ),
        compiler_params=pltpu.CompilerParams(vmem_limit_bytes=mib << 20),
    )


def on_device(local_weights, outer_base, momentum, error_feedback, q_start, tokens):
    replicas, shards = lax.axis_size(peers), lax.axis_size(shard)
    rows, kv = outer_base.shape
    rank = q_start.shape[1]
    own = rows // replicas
    cols = kv // replicas
    core = lax.axis_index("core")
    base = outer_base.astype(f32)
    own_tokens = tokens[0]
    block = own_tokens.shape[0] // shards
    shape = jax.ShapeDtypeStruct

    my_momentum = copy_for_each(momentum.T, chips)

    pseudo = base - local_weights[0].astype(f32) + error_feedback[0].astype(f32)
    halves = pseudo.reshape(2, rows // 2, kv)
    pair = swap(pick(halves, 1 - core, 0), "core")
    pair = (pick(halves, core, 0) + pair).astype(bf16)
    pair, my_momentum = lax.optimization_barrier((pair, my_momentum))
    first = exchange(pair.reshape(replicas // 2, own, kv), chips)
    lanes = 4 * rank
    (second,) = in_vmem(
        functools.partial(moments, own=own, rank=rank, replicas=replicas),
        (shape((replicas, own, lanes), f32),),
        2,
        6,
        40000000,
        (pltpu.VMEM((replicas, own, lanes), f32),),
        1,
    )(first, q_start.T)
    second = exchange(second, peers)

    its_momentum = swap(my_momentum, "core")
    full_momentum = jnp.stack(
        [
            jnp.where(core == 0, my_momentum, its_momentum),
            jnp.where(core == 0, its_momentum, my_momentum),
        ],
        axis=1,
    ).reshape(kv, rows)
    full_momentum = full_momentum.T

    part = (shards // 2, block, kv // 2)
    left, right, keep = in_vmem(
        key_products,
        (shape(part, bf16), shape(part, bf16), shape((*part[:2], kv), f32)),
        3,
        12,
        2 * tokens.shape[1] * rows * kv,
        (pltpu.VMEM((*part[:2], kv), bf16), pltpu.SemaphoreType.DMA((2,))),
        2,
    )(own_tokens, outer_base, full_momentum)
    across = ("y2", "y1", "y0")
    left = lax.ppermute(left, across, [(i, i ^ 1) for i in range(8)])
    right = lax.ppermute(
        right, across, [(i, (i + 1 if i % 2 else i - 1) % 8) for i in range(8)]
    )
    key_part = keep + jnp.concatenate([left, right], axis=-1).astype(f32)
    key_part = halve(key_part.reshape(4, 2, block, kv), "xl", 1)
    key_part = key_part.reshape(2, 2, block, kv)
    key_part = halve(key_part, "y1", 1)
    key_sum = halve(key_part, "y2", 0)

    tall = (shards, own + block // 4, lanes)
    (third,) = in_vmem(
        functools.partial(token_products, own=own, rank=rank),
        (shape(tall, f32),),
        2,
        12,
        500000000,
        (pltpu.VMEM(tall, f32),),
        1,
    )(second, own_tokens)
    third = exchange(third, shard)
    copies, total = in_vmem(
        shard_sums,
        (shape((replicas, own, lanes), f32), shape(third.shape[1:], f32)),
        1,
        4,
        1000000,
        (pltpu.VMEM((replicas, own, lanes), f32),),
        1,
    )(third)
    fourth = exchange(copies, peers)
    basis, token_basis, inverse = in_vmem(
        functools.partial(bases, own=own, rank=rank),
        (
            shape((rows, lanes), f32),
            shape((block, lanes), f32),
            shape((lanes, lanes), f32),
        ),
        2,
        6,
        100000000,
    )(total, second)
    new_base, new_momentum, new_error, key_low = in_vmem(
        outputs,
        (
            shape((rows, kv), bf16),
            shape((cols, rows), bf16),
            shape((rows, kv), bf16),
            shape((block, kv), f32),
        ),
        9,
        12,
        400000000,
        (pltpu.VMEM((kv, lanes), f32),),
    )(
        fourth,
        inverse,
        basis,
        token_basis,
        local_weights[0],
        outer_base,
        error_feedback[0],
        full_momentum,
        momentum.T,
    )
    key_rows = (key_sum - key_low).astype(bf16)
    return new_base, new_momentum.T, new_error[None], key_rows[None]


def solution(mesh):
    fine = Mesh(
        mesh.devices.reshape(8, 2, 2, 2, 2, 2, 2), chips + ("core",) + shard
    )
    replica = chips + ("core",)
    in_specs = (
        P(replica, shard, None),
        P(shard, None),
        P(shard, replica),
        P(replica, shard, None),
        P(),
        P(replica, None, shard),
    )
    out_specs = (
        P(shard, None),
        P(shard, replica),
        P(replica, shard, None),
        P(replica, shard, None),
    )

    def step(*arrays):
        return on_device(*arrays)

    step = jax.shard_map(
        step, mesh=fine, in_specs=in_specs, out_specs=out_specs, check_vma=False
    )
    return step
```

```python
import functools

import jax
import jax.numpy as jnp
from jax import lax
from jax.experimental import pallas as pl
from jax.experimental.pallas import tpu as pltpu
from jax.sharding import Mesh, PartitionSpec as P


outer_mu = 0.9
outer_rate = 0.7
own_mom = outer_rate * outer_mu * outer_mu
own_upd = outer_rate * (outer_mu + 1.0)


chips = ("z", "xh")
peers = ("core", "z", "xh")
shard = ("y2", "y1", "y0", "xl")
f32, bf16 = jnp.float32, jnp.bfloat16
highest = lax.Precision.HIGHEST


def swap(x, axis):
    return lax.ppermute(x, axis, [(0, 1), (1, 0)])


def exchange(x, axis):
    return lax.all_to_all(x, axis, 0, 0, tiled=True)


def dot(a, b, dims, precision=None):
    return lax.dot_general(
        a, b, (dims, ((), ())), precision=precision, preferred_element_type=f32
    )


def lane_group(shape, rank):
    return lax.broadcasted_iota(jnp.int32, shape, 1) // rank


def moments(first_ref, q_ref, hbm_ref, out_ref, *, own, rank, replicas):
    mean = jnp.sum(first_ref[:, :own].astype(f32), axis=0) * (1.0 / replicas)
    q = jnp.concatenate([q_ref[...]] * 4, axis=0)
    p = dot(mean, q, ((1,), (1,)), highest)
    group = lane_group(p.shape, rank)
    p_at = [jnp.where(group == i, p, 0.0) for i in range(4)]
    upper = dot(p_at[0], p_at[1], ((0,), (0,)), highest)
    lower = dot(p_at[0], p_at[2], ((0,), (0,)), highest)
    same = p_at[0] + upper[:own] + lower[own : 2 * own]
    q_rows = dot(mean, p_at[3], ((0,), (0,)), highest)
    out_ref[...] = q_rows.reshape(out_ref.shape) + same[None]
    pltpu.sync_copy(out_ref, hbm_ref)


def token_products(second_ref, tokens_ref, hbm_ref, out_ref, *, own, rank):
    peers_, rows_, lanes = second_ref.shape
    shards = out_ref.shape[0]
    block = tokens_ref.shape[0] // shards
    step = block // 4
    second = second_ref[...]
    sums = jnp.sum(second, axis=0)
    flat = second.reshape(peers_ * rows_, lanes)
    p = jnp.where(lane_group(flat.shape, rank) == 0, flat, 0.0)
    total = jnp.zeros((shards * step, lanes), f32)
    tokens = tokens_ref[...].reshape(shards, 4, step, -1)
    for i in range(4):
        at = pltpu.roll(p, i * rank, 1) if i else p
        high = at.astype(bf16)
        low = (at - high.astype(f32)).astype(bf16)
        part = tokens[:, i].reshape(shards * step, -1)
        total = total + dot(part, high, ((1,), (0,))) + dot(part, low, ((1,), (0,)))
    out_ref[:, :own] = jnp.broadcast_to(sums[None], (shards, own, lanes))
    out_ref[:, own:] = total.reshape(shards, step, lanes)
    pltpu.sync_copy(out_ref, hbm_ref)


def pseudo_halves(
    local_hbm, base_hbm, error_hbm, send_ref, keep_ref, local_ref, base_ref, error_ref, sems
):
    core = lax.axis_index("core")
    half = keep_ref.shape[0]
    pairs = ((local_hbm, local_ref), (base_hbm, base_ref), (error_hbm, error_ref))
    for i, (src, dst) in enumerate(pairs):
        pltpu.make_async_copy(src, dst, sems.at[i]).start()
    for i, (src, dst) in enumerate(pairs):
        pltpu.make_async_copy(src, dst, sems.at[i]).wait()

    def pseudo(which):
        at = pl.ds(pl.multiple_of(which * half, half), half)
        base, local = base_ref[at].astype(f32), local_ref[at].astype(f32)
        return base - local + error_ref[at].astype(f32)

    send_ref[...] = pseudo(1 - core)
    keep_ref[...] = pseudo(core)


def key_products(
    tokens_ref, base_ref, first_ref, its_ref,
    left_ref, right_ref, kept_ref, full_ref, sent, keep, sems,
):
    y0, core = lax.axis_index("y0"), lax.axis_index("core")
    mine = first_ref[:, its_ref.shape[1] :].astype(f32)
    other = its_ref[...].astype(f32)
    pairs = jnp.concatenate(
        [
            jnp.where(core == 0, mine, other)[:, None],
            jnp.where(core == 0, other, mine)[:, None],
        ],
        axis=1,
    )
    momentum = pairs.reshape(base_ref.shape[1], base_ref.shape[0]).T
    full_ref[...] = momentum.astype(bf16)
    settled = (base_ref[...].astype(f32) - own_mom * momentum).astype(bf16)
    groups, block, cols = keep.shape[0] // 2, keep.shape[1], keep.shape[2]
    half = cols // 2

    def product(i, parity):
        at = pl.multiple_of((2 * i + parity) * 2 * block, 2 * block)
        part = dot(tokens_ref[pl.ds(at, 2 * block)], settled, ((1,), (0,)))
        return part.reshape(2, block, cols)

    for i in range(groups):
        sent[2 * i : 2 * i + 2] = product(i, 1 - y0).astype(bf16)
    copies = [
        pltpu.make_async_copy(sent.at[:, :, :half], left_ref, sems.at[0]),
        pltpu.make_async_copy(sent.at[:, :, half:], right_ref, sems.at[1]),
        pltpu.make_async_copy(keep, kept_ref, sems.at[2]),
    ]
    for copy in copies[:2]:
        copy.start()
    for i in range(groups):
        keep[2 * i : 2 * i + 2] = product(i, y0)
    copies[2].start()
    for copy in copies:
        copy.wait()


def fold(*refs, axis, n):
    came_ref, kept_ref, send_ref, keep_ref = refs[:n], refs[n], refs[n + 1], refs[n + 2]
    came, held, sent, sems = refs[n + 3 : 2 * n + 3], *refs[2 * n + 3 :]
    me = lax.axis_index(axis)
    halves = (1 - me, me)
    loads = [
        [
            pltpu.make_async_copy(
                src.at[:, half], dst.at[:, i], sems.at[i * (n + 1) + j]
            )
            for j, (src, dst) in enumerate(zip((*came_ref, kept_ref), (*came, held)))
        ]
        for i, half in enumerate(halves)
    ]
    for load in loads[0] + loads[1]:
        load.start()
    out = [
        pltpu.make_async_copy(sent, send_ref, sems.at[2 * n + 2]),
        pltpu.make_async_copy(held.at[:, 1], keep_ref, sems.at[2 * n + 3]),
    ]
    for i in range(2):
        for load in loads[i]:
            load.wait()
        at, width = 0, held.shape[-1] // n
        for part in came:
            here = slice(at, at + width)
            total = held[:, i, :, here] + part[:, i].astype(f32)
            if i == 0:
                sent[:, :, here] = total.astype(bf16)
            else:
                held[:, i, :, here] = total
            at += width
        out[i].start()
    for copy in out:
        copy.wait()


def fold_call(came, kept, axis):
    groups, _, block, cols = kept.shape
    n = len(came)
    hbm = pl.BlockSpec(memory_space=pltpu.HBM)
    shape = jax.ShapeDtypeStruct
    return pl.pallas_call(
        functools.partial(fold, axis=axis, n=n),
        out_shape=(
            shape((groups, block, cols), bf16),
            shape((groups, block, cols), f32),
        ),
        in_specs=[hbm] * (n + 1),
        out_specs=(hbm, hbm),
        scratch_shapes=(
            *[pltpu.VMEM(c.shape, bf16) for c in came],
            pltpu.VMEM(kept.shape, f32),
            pltpu.VMEM((groups, block, cols), bf16),
            pltpu.SemaphoreType.DMA((2 * n + 4,)),
        ),
        cost_estimate=pl.CostEstimate(
            flops=kept.size, bytes_accessed=kept.size * 6, transcendentals=0
        ),
    )(*came, kept)


def shard_sums(third_ref, hbm_ref, total_ref, copies_ref):
    total = jnp.sum(third_ref[...], axis=0)
    total_ref[...] = total
    copies_ref[...] = jnp.broadcast_to(
        total[None, : copies_ref.shape[1]], copies_ref.shape
    )
    pltpu.sync_copy(copies_ref, hbm_ref)


def bases(total_ref, second_ref, basis_ref, token_ref, inverse_ref, *, own, rank):
    total = total_ref[...]
    lanes = total.shape[1]
    sums, token_sum = total[:own], total[own:]
    left = jnp.concatenate(
        [pltpu.roll(sums, lanes - rank, 1), pltpu.roll(sums, lanes - 2 * rank, 1)], axis=0
    )
    row = lax.broadcasted_iota(jnp.int32, (rank, lanes), 0)
    lane = lax.broadcasted_iota(jnp.int32, (rank, lanes), 1)
    work = jnp.where(lane < rank, left, jnp.where(lane == row + rank, 1.0, 0.0))
    for j in range(rank - 1):
        ratio = work[:, j : j + 1] / work[j : j + 1, j : j + 1]
        work = work - jnp.where(row > j, ratio * work[j : j + 1], 0.0)
    pivot = jnp.sum(jnp.where(lane == row, work, 0.0), axis=1, keepdims=True)
    work = jnp.where((lane >= rank) & (lane < 2 * rank), work / jnp.sqrt(pivot), 0.0)
    rest = jnp.zeros((lanes - rank, lanes), f32)
    at = [
        jnp.concatenate([pltpu.roll(work, ((i - 1) * rank) % lanes, 1), rest], axis=0)
        for i in (0, 2, 3)
    ]
    at.insert(1, jnp.concatenate([work, rest], axis=0))
    flat = second_ref[...].reshape(-1, lanes)
    basis_ref[...] = dot(flat, at[0], ((1,), (1,)), highest)
    token_ref[...] = jnp.concatenate(
        [dot(token_sum, a, ((1,), (1,)), highest) for a in at], axis=0
    )
    inverse_ref[...] = at[3]


def outputs(
    fourth_ref, inverse_ref, basis_ref, token_ref, local_ref, base_ref, error_ref,
    full_ref, momentum_ref, base_out, momentum_out, error_out, key_out, q_scratch,
):
    last = ((1,), (1,))
    rows_, cols = base_ref.shape[0], momentum_ref.shape[0]
    flat = fourth_ref[...].reshape(-1, fourth_ref.shape[2])
    q = dot(flat, inverse_ref[...], last, highest)
    q_scratch[...] = q
    key_out[...] = own_upd * dot(token_ref[...], q, last, highest)
    at = lax.axis_index(chips + ("core",)) * cols
    own_q = q_scratch[pl.ds(pl.multiple_of(at, cols), cols)]
    momentum_out[...] = (
        outer_mu * momentum_ref[...].astype(f32)
        + dot(own_q, basis_ref[...], last, highest)
    ).astype(bf16)
    step = rows_ // 4
    for i in range(4):
        here = slice(i * step, (i + 1) * step)
        update = dot(basis_ref[here], q, last, highest)
        base = base_ref[here].astype(f32)
        pseudo = base - local_ref[here].astype(f32) + error_ref[here].astype(f32)
        error_out[here] = (pseudo - update).astype(bf16)
        moment = outer_mu * full_ref[here].astype(f32) + update
        base_out[here] = (base - outer_rate * (outer_mu * moment + update)).astype(bf16)


def in_vmem(kernel, out_shape, n, mib, flops, scratch=(), far=0, far_in=False):
    whole = pl.BlockSpec(memory_space=pltpu.VMEM)
    hbm = pl.BlockSpec(memory_space=pltpu.HBM)
    return pl.pallas_call(
        kernel,
        out_shape=out_shape,
        in_specs=[hbm if far_in else whole] * n,
        out_specs=tuple(hbm if i < far else whole for i in range(len(out_shape))),
        scratch_shapes=scratch,
        cost_estimate=pl.CostEstimate(
            flops=flops, bytes_accessed=flops // 100, transcendentals=0
        ),
        compiler_params=pltpu.CompilerParams(vmem_limit_bytes=mib << 20),
    )


def on_device(local_weights, outer_base, momentum, error_feedback, q_start, tokens):
    replicas, shards = lax.axis_size(peers), lax.axis_size(shard)
    rows, kv = outer_base.shape
    rank = q_start.shape[1]
    own = rows // replicas
    cols = kv // replicas
    own_tokens = tokens[0]
    block = own_tokens.shape[0] // shards
    shape = jax.ShapeDtypeStruct

    half = shape((rows // 2, kv), f32)
    given = pltpu.VMEM((rows, kv), bf16)
    send, pair = in_vmem(
        pseudo_halves,
        (half, half),
        3,
        8,
        1000000,
        (given, given, given, pltpu.SemaphoreType.DMA((3,))),
        far_in=True,
    )(local_weights[0], outer_base, error_feedback[0])
    send = swap(send, "core")
    pair = (pair + send).astype(bf16)
    first = exchange(
        jnp.concatenate(
            [
                pair.reshape(replicas // 2, own, kv),
                jnp.broadcast_to(momentum.T, (replicas // 2, cols, rows)),
            ],
            axis=1,
        ),
        chips,
    )
    lanes = 4 * rank
    (second,) = in_vmem(
        functools.partial(moments, own=own, rank=rank, replicas=replicas),
        (shape((replicas, own, lanes), f32),),
        2,
        6,
        40000000,
        (pltpu.VMEM((replicas, own, lanes), f32),),
        1,
    )(first, q_start.T)
    second = exchange(second, peers)

    its_momentum = swap(first[:, own:], "core")

    part = (shards // 2, block, kv // 2)
    whole = (*part[:2], kv)
    left, right, kept, full_momentum = in_vmem(
        key_products,
        (shape(part, bf16), shape(part, bf16), shape(whole, f32), shape((rows, kv), bf16)),
        4,
        16,
        2 * tokens.shape[1] * rows * kv,
        (
            pltpu.VMEM(whole, bf16),
            pltpu.VMEM(whole, f32),
            pltpu.SemaphoreType.DMA((3,)),
        ),
        3,
    )(own_tokens, outer_base, first, its_momentum)
    across = ("y2", "y1", "y0")
    left = lax.ppermute(left, across, [(i, i ^ 1) for i in range(8)])
    right = lax.ppermute(
        right, across, [(i, (i + 1 if i % 2 else i - 1) % 8) for i in range(8)]
    )
    for axis, groups, came in (
        ("xl", 4, (left, right)), ("y1", 2, None), ("y2", 1, None)
    ):
        view = (groups, 2, block)
        send, kept = fold_call(
            [c.reshape(*view, -1) for c in came or (send,)],
            kept.reshape(*view, kv),
            axis,
        )
        send = swap(send, axis)

    tall = (shards, own + block // 4, lanes)
    (third,) = in_vmem(
        functools.partial(token_products, own=own, rank=rank),
        (shape(tall, f32),),
        2,
        12,
        500000000,
        (pltpu.VMEM(tall, f32),),
        1,
    )(second, own_tokens)
    third = exchange(third, shard)
    copies, total = in_vmem(
        shard_sums,
        (shape((replicas, own, lanes), f32), shape(third.shape[1:], f32)),
        1,
        4,
        1000000,
        (pltpu.VMEM((replicas, own, lanes), f32),),
        1,
    )(third)
    fourth = exchange(copies, peers)
    basis, token_basis, inverse = in_vmem(
        functools.partial(bases, own=own, rank=rank),
        (
            shape((rows, lanes), f32),
            shape((block, lanes), f32),
            shape((lanes, lanes), f32),
        ),
        2,
        6,
        100000000,
    )(total, second)
    new_base, new_momentum, new_error, key_low = in_vmem(
        outputs,
        (
            shape((rows, kv), bf16),
            shape((cols, rows), bf16),
            shape((rows, kv), bf16),
            shape((block, kv), f32),
        ),
        9,
        12,
        400000000,
        (pltpu.VMEM((kv, lanes), f32),),
    )(
        fourth,
        inverse,
        basis,
        token_basis,
        local_weights[0],
        outer_base,
        error_feedback[0],
        full_momentum,
        momentum.T,
    )
    key_rows = (kept[0] + send[0].astype(f32) - key_low).astype(bf16)
    return new_base, new_momentum.T, new_error[None], key_rows[None]


def solution(mesh):
    fine = Mesh(
        mesh.devices.reshape(8, 2, 2, 2, 2, 2, 2), chips + ("core",) + shard
    )
    replica = chips + ("core",)
    in_specs = (
        P(replica, shard, None),
        P(shard, None),
        P(shard, replica),
        P(replica, shard, None),
        P(),
        P(replica, None, shard),
    )
    out_specs = (
        P(shard, None),
        P(shard, replica),
        P(replica, shard, None),
        P(replica, shard, None),
    )

    def step(*arrays):
        return on_device(*arrays)

    step = jax.shard_map(
        step, mesh=fine, in_specs=in_specs, out_specs=out_specs, check_vma=False
    )
    return step
```

```python
import functools

import jax
import jax.numpy as jnp
from jax import lax
from jax.experimental import pallas as pl
from jax.experimental.pallas import tpu as pltpu
from jax.sharding import Mesh, PartitionSpec as P


outer_mu = 0.9
outer_rate = 0.7
own_mom = outer_rate * outer_mu * outer_mu
own_upd = outer_rate * (outer_mu + 1.0)


chips = ("z", "xh")
peers = ("core", "z", "xh")
shard = ("y2", "y1", "y0", "xl")
f32, bf16 = jnp.float32, jnp.bfloat16
highest = lax.Precision.HIGHEST


def swap(x, axis):
    return lax.ppermute(x, axis, [(0, 1), (1, 0)])


def exchange(x, axis):
    return lax.all_to_all(x, axis, 0, 0, tiled=True)


def dot(a, b, dims, precision=None):
    return lax.dot_general(
        a, b, (dims, ((), ())), precision=precision, preferred_element_type=f32
    )


def lane_group(shape, rank):
    return lax.broadcasted_iota(jnp.int32, shape, 1) // rank


def moments(first_ref, q_ref, hbm_ref, out_ref, *, own, rank, replicas):
    mean = jnp.sum(first_ref[:, :own].astype(f32), axis=0) * (1.0 / replicas)
    q = jnp.concatenate([q_ref[...]] * 4, axis=0)
    p = dot(mean, q, ((1,), (1,)), highest)
    group = lane_group(p.shape, rank)
    p_at = [jnp.where(group == i, p, 0.0) for i in range(4)]
    upper = dot(p_at[0], p_at[1], ((0,), (0,)), highest)
    lower = dot(p_at[0], p_at[2], ((0,), (0,)), highest)
    same = p_at[0] + upper[:own] + lower[own : 2 * own]
    q_rows = dot(mean, p_at[3], ((0,), (0,)), highest)
    out_ref[...] = q_rows.reshape(out_ref.shape) + same[None]
    pltpu.sync_copy(out_ref, hbm_ref)


def token_products(second_ref, tokens_ref, hbm_ref, out_ref, *, own, rank):
    peers_, rows_, lanes = second_ref.shape
    shards = out_ref.shape[0]
    block = tokens_ref.shape[0] // shards
    step = block // 4
    second = second_ref[...]
    sums = jnp.sum(second, axis=0)
    flat = second.reshape(peers_ * rows_, lanes)
    p = jnp.where(lane_group(flat.shape, rank) == 0, flat, 0.0)
    total = jnp.zeros((shards * step, lanes), f32)
    tokens = tokens_ref[...].reshape(shards, 4, step, -1)
    for i in range(4):
        at = pltpu.roll(p, i * rank, 1) if i else p
        high = at.astype(bf16)
        low = (at - high.astype(f32)).astype(bf16)
        part = tokens[:, i].reshape(shards * step, -1)
        total = total + dot(part, high, ((1,), (0,))) + dot(part, low, ((1,), (0,)))
    out_ref[:, :own] = jnp.broadcast_to(sums[None], (shards, own, lanes))
    out_ref[:, own:] = total.reshape(shards, step, lanes)
    pltpu.sync_copy(out_ref, hbm_ref)


def pseudo_halves(
    local_hbm, base_hbm, error_hbm, momentum_hbm, send_ref, keep_ref,
    local_ref, base_ref, error_ref, momentum_ref, sems,
):
    core = lax.axis_index("core")
    half = keep_ref.shape[0]
    pairs = (
        (local_hbm, local_ref),
        (base_hbm, base_ref),
        (error_hbm, error_ref),
        (momentum_hbm, momentum_ref),
    )
    for i, (src, dst) in enumerate(pairs):
        pltpu.make_async_copy(src, dst, sems.at[i]).start()
    for i, (src, dst) in enumerate(pairs):
        pltpu.make_async_copy(src, dst, sems.at[i]).wait()

    def pseudo(which):
        at = pl.ds(pl.multiple_of(which * half, half), half)
        base, local = base_ref[at].astype(f32), local_ref[at].astype(f32)
        return base - local + error_ref[at].astype(f32)

    send_ref[:half] = pseudo(1 - core)
    send_ref[half:] = momentum_ref[...].astype(f32)
    keep_ref[...] = pseudo(core)


def key_products(
    tokens_ref, base_ref, first_ref,
    left_ref, right_ref, kept_ref, full_ref, sent, keep, sems, *, own,
):
    y0 = lax.axis_index("y0")
    momentum = first_ref[:, own:].reshape(base_ref.shape[1], base_ref.shape[0])
    momentum = momentum.astype(f32).T
    full_ref[...] = momentum.astype(bf16)
    settled = (base_ref[...].astype(f32) - own_mom * momentum).astype(bf16)
    groups, block, cols = keep.shape[0] // 2, keep.shape[1], keep.shape[2]
    half = cols // 2

    def product(i, parity):
        at = pl.multiple_of((2 * i + parity) * 2 * block, 2 * block)
        part = dot(tokens_ref[pl.ds(at, 2 * block)], settled, ((1,), (0,)))
        return part.reshape(2, block, cols)

    for i in range(groups):
        sent[2 * i : 2 * i + 2] = product(i, 1 - y0).astype(bf16)
    copies = [
        pltpu.make_async_copy(sent.at[:, :, :half], left_ref, sems.at[0]),
        pltpu.make_async_copy(sent.at[:, :, half:], right_ref, sems.at[1]),
        pltpu.make_async_copy(keep, kept_ref, sems.at[2]),
    ]
    for copy in copies[:2]:
        copy.start()
    for i in range(groups):
        keep[2 * i : 2 * i + 2] = product(i, y0)
    copies[2].start()
    for copy in copies:
        copy.wait()


def fold(*refs, axis, n):
    came, kept_ref, send_ref, keep_ref = refs[:n], *refs[n:]
    me = lax.axis_index(axis)
    width = kept_ref.shape[-1] // n
    for g in range(kept_ref.shape[0]):
        for i, part in enumerate(came):
            at = slice(i * width, (i + 1) * width)
            send_ref[g, :, at] = (
                kept_ref[g, 1 - me, :, at] + part[g, 1 - me].astype(f32)
            ).astype(bf16)
            keep_ref[g, :, at] = kept_ref[g, me, :, at] + part[g, me].astype(f32)


def fold_call(came, kept, axis):
    groups, _, block, cols = kept.shape
    shape = jax.ShapeDtypeStruct
    return in_vmem(
        functools.partial(fold, axis=axis, n=len(came)),
        (shape((groups, block, cols), bf16), shape((groups, block, cols), f32)),
        len(came) + 1,
        12,
        kept.size,
    )(*came, kept)


def shard_sums(third_ref, hbm_ref, total_ref, copies_ref):
    total = jnp.sum(third_ref[...], axis=0)
    total_ref[...] = total
    copies_ref[...] = jnp.broadcast_to(
        total[None, : copies_ref.shape[1]], copies_ref.shape
    )
    pltpu.sync_copy(copies_ref, hbm_ref)


def bases(total_ref, second_ref, basis_ref, token_ref, inverse_ref, *, own, rank):
    total = total_ref[...]
    lanes = total.shape[1]
    sums, token_sum = total[:own], total[own:]
    left = jnp.concatenate(
        [pltpu.roll(sums, lanes - rank, 1), pltpu.roll(sums, lanes - 2 * rank, 1)], axis=0
    )
    row = lax.broadcasted_iota(jnp.int32, (rank, lanes), 0)
    lane = lax.broadcasted_iota(jnp.int32, (rank, lanes), 1)
    work = jnp.where(lane < rank, left, jnp.where(lane == row + rank, 1.0, 0.0))
    for j in range(rank - 1):
        ratio = work[:, j : j + 1] / work[j : j + 1, j : j + 1]
        work = work - jnp.where(row > j, ratio * work[j : j + 1], 0.0)
    pivot = jnp.sum(jnp.where(lane == row, work, 0.0), axis=1, keepdims=True)
    work = jnp.where((lane >= rank) & (lane < 2 * rank), work / jnp.sqrt(pivot), 0.0)
    rest = jnp.zeros((lanes - rank, lanes), f32)
    at = [
        jnp.concatenate([pltpu.roll(work, ((i - 1) * rank) % lanes, 1), rest], axis=0)
        for i in (0, 2, 3)
    ]
    at.insert(1, jnp.concatenate([work, rest], axis=0))
    flat = second_ref[...].reshape(-1, lanes)
    basis_ref[...] = dot(flat, at[0], ((1,), (1,)), highest)
    token_ref[...] = jnp.concatenate(
        [dot(token_sum, a, ((1,), (1,)), highest) for a in at], axis=0
    )
    inverse_ref[...] = at[3]


def outputs(
    fourth_ref, inverse_ref, basis_ref, token_ref, local_ref, base_ref, error_ref,
    full_ref, momentum_ref, base_out, momentum_out, error_out, key_out, q_scratch,
):
    last = ((1,), (1,))
    rows_, cols = base_ref.shape[0], momentum_ref.shape[0]
    flat = fourth_ref[...].reshape(-1, fourth_ref.shape[2])
    q = dot(flat, inverse_ref[...], last, highest)
    q_scratch[...] = q
    key_out[...] = own_upd * dot(token_ref[...], q, last, highest)
    at = lax.axis_index(chips + ("core",)) * cols
    own_q = q_scratch[pl.ds(pl.multiple_of(at, cols), cols)]
    momentum_out[...] = (
        outer_mu * momentum_ref[...].astype(f32)
        + dot(own_q, basis_ref[...], last, highest)
    ).astype(bf16)
    step = rows_ // 4
    for i in range(4):
        here = slice(i * step, (i + 1) * step)
        update = dot(basis_ref[here], q, last, highest)
        base = base_ref[here].astype(f32)
        pseudo = base - local_ref[here].astype(f32) + error_ref[here].astype(f32)
        error_out[here] = (pseudo - update).astype(bf16)
        moment = outer_mu * full_ref[here].astype(f32) + update
        base_out[here] = (base - outer_rate * (outer_mu * moment + update)).astype(bf16)


def in_vmem(kernel, out_shape, n, mib, flops, scratch=(), far=0, far_in=False):
    whole = pl.BlockSpec(memory_space=pltpu.VMEM)
    hbm = pl.BlockSpec(memory_space=pltpu.HBM)
    return pl.pallas_call(
        kernel,
        out_shape=out_shape,
        in_specs=[hbm if far_in else whole] * n,
        out_specs=tuple(hbm if i < far else whole for i in range(len(out_shape))),
        scratch_shapes=scratch,
        cost_estimate=pl.CostEstimate(
            flops=flops, bytes_accessed=flops // 100, transcendentals=0
        ),
        compiler_params=pltpu.CompilerParams(vmem_limit_bytes=(mib << 20) or None),
    )


def on_device(local_weights, outer_base, momentum, error_feedback, q_start, tokens):
    replicas, shards = lax.axis_size(peers), lax.axis_size(shard)
    rows, kv = outer_base.shape
    rank = q_start.shape[1]
    own = rows // replicas
    cols = kv // replicas
    core = lax.axis_index("core")
    own_tokens = tokens[0]
    block = own_tokens.shape[0] // shards
    shape = jax.ShapeDtypeStruct

    half = rows // 2
    given = pltpu.VMEM((rows, kv), bf16)
    send, pair = in_vmem(
        pseudo_halves,
        (shape((half + cols, kv), f32), shape((half, kv), f32)),
        4,
        0,
        1000000,
        (
            given,
            given,
            given,
            pltpu.VMEM((cols, rows), bf16),
            pltpu.SemaphoreType.DMA((4,)),
        ),
        far_in=True,
    )(local_weights[0], outer_base, error_feedback[0], momentum.T)
    came = swap(send, "core")
    pair = (pair + came[:half]).astype(bf16)
    mine, its = momentum.T, came[half:].astype(bf16)
    core = lax.axis_index("core")
    both = jnp.concatenate(
        [jnp.where(core == 0, mine, its), jnp.where(core == 0, its, mine)], axis=0
    )
    first = exchange(
        jnp.concatenate(
            [
                pair.reshape(replicas // 2, own, kv),
                jnp.broadcast_to(both, (replicas // 2, 2 * cols, rows)),
            ],
            axis=1,
        ),
        chips,
    )
    lanes = 4 * rank
    (second,) = in_vmem(
        functools.partial(moments, own=own, rank=rank, replicas=replicas),
        (shape((replicas, own, lanes), f32),),
        2,
        6,
        40000000,
        (pltpu.VMEM((replicas, own, lanes), f32),),
        1,
    )(first, q_start.T)
    second = exchange(second, peers)

    part = (shards // 2, block, kv // 2)
    whole = (*part[:2], kv)
    left, right, kept, full_momentum = in_vmem(
        functools.partial(key_products, own=own),
        (shape(part, bf16), shape(part, bf16), shape(whole, f32), shape((rows, kv), bf16)),
        3,
        16,
        2 * tokens.shape[1] * rows * kv,
        (
            pltpu.VMEM(whole, bf16),
            pltpu.VMEM(whole, f32),
            pltpu.SemaphoreType.DMA((3,)),
        ),
        3,
    )(own_tokens, outer_base, first)
    across = ("y2", "y1", "y0")
    left = lax.ppermute(left, across, [(i, i ^ 1) for i in range(8)])
    right = lax.ppermute(
        right, across, [(i, (i + 1 if i % 2 else i - 1) % 8) for i in range(8)]
    )
    for axis, groups, came in (
        ("xl", 4, (left, right)), ("y1", 2, None), ("y2", 1, None)
    ):
        view = (groups, 2, block)
        send, kept = fold_call(
            [c.reshape(*view, -1) for c in came or (send,)],
            kept.reshape(*view, kv),
            axis,
        )
        send = swap(send, axis)

    tall = (shards, own + block // 4, lanes)
    (third,) = in_vmem(
        functools.partial(token_products, own=own, rank=rank),
        (shape(tall, f32),),
        2,
        12,
        500000000,
        (pltpu.VMEM(tall, f32),),
        1,
    )(second, own_tokens)
    third = exchange(third, shard)
    copies, total = in_vmem(
        shard_sums,
        (shape((replicas, own, lanes), f32), shape(third.shape[1:], f32)),
        1,
        4,
        1000000,
        (pltpu.VMEM((replicas, own, lanes), f32),),
        1,
    )(third)
    fourth = exchange(copies, peers)
    basis, token_basis, inverse = in_vmem(
        functools.partial(bases, own=own, rank=rank),
        (
            shape((rows, lanes), f32),
            shape((block, lanes), f32),
            shape((lanes, lanes), f32),
        ),
        2,
        6,
        100000000,
    )(total, second)
    new_base, new_momentum, new_error, key_low = in_vmem(
        outputs,
        (
            shape((rows, kv), bf16),
            shape((cols, rows), bf16),
            shape((rows, kv), bf16),
            shape((block, kv), f32),
        ),
        9,
        12,
        400000000,
        (pltpu.VMEM((kv, lanes), f32),),
    )(
        fourth,
        inverse,
        basis,
        token_basis,
        local_weights[0],
        outer_base,
        error_feedback[0],
        full_momentum,
        momentum.T,
    )
    key_rows = (kept[0] + send[0].astype(f32) - key_low).astype(bf16)
    return new_base, new_momentum.T, new_error[None], key_rows[None]


def solution(mesh):
    fine = Mesh(
        mesh.devices.reshape(8, 2, 2, 2, 2, 2, 2), chips + ("core",) + shard
    )
    replica = chips + ("core",)
    in_specs = (
        P(replica, shard, None),
        P(shard, None),
        P(shard, replica),
        P(replica, shard, None),
        P(),
        P(replica, None, shard),
    )
    out_specs = (
        P(shard, None),
        P(shard, replica),
        P(replica, shard, None),
        P(replica, shard, None),
    )

    def step(*arrays):
        return on_device(*arrays)

    step = jax.shard_map(
        step, mesh=fine, in_specs=in_specs, out_specs=out_specs, check_vma=False
    )
    return step
```

```python
import functools

import jax
import jax.numpy as jnp
from jax import lax
from jax.experimental import pallas as pl
from jax.experimental.pallas import tpu as pltpu
from jax.sharding import Mesh, PartitionSpec as P


outer_mu = 0.9
outer_rate = 0.7
own_mom = outer_rate * outer_mu * outer_mu
own_upd = outer_rate * (outer_mu + 1.0)


chips = ("z", "xh")
peers = ("core", "z", "xh")
shard = ("y2", "y1", "y0", "xl")
f32, bf16 = jnp.float32, jnp.bfloat16
highest = lax.Precision.HIGHEST


def swap(x, axis):
    return lax.ppermute(x, axis, [(0, 1), (1, 0)])


def exchange(x, axis):
    return lax.all_to_all(x, axis, 0, 0, tiled=True)


def dot(a, b, dims, precision=None):
    return lax.dot_general(
        a, b, (dims, ((), ())), precision=precision, preferred_element_type=f32
    )


def lane_group(shape, rank):
    return lax.broadcasted_iota(jnp.int32, shape, 1) // rank


def moments(first_ref, q_ref, hbm_ref, out_ref, *, own, rank, replicas):
    mean = jnp.sum(first_ref[:, :own].astype(f32), axis=0) * (1.0 / replicas)
    q = jnp.concatenate([q_ref[...]] * 4, axis=0)
    p = dot(mean, q, ((1,), (1,)), highest)
    group = lane_group(p.shape, rank)
    p_at = [jnp.where(group == i, p, 0.0) for i in range(4)]
    upper = dot(p_at[0], p_at[1], ((0,), (0,)), highest)
    lower = dot(p_at[0], p_at[2], ((0,), (0,)), highest)
    same = p_at[0] + upper[:own] + lower[own : 2 * own]
    q_rows = dot(mean, p_at[3], ((0,), (0,)), highest)
    out_ref[...] = q_rows.reshape(out_ref.shape) + same[None]
    pltpu.sync_copy(out_ref, hbm_ref)


def token_products(second_ref, tokens_ref, hbm_ref, out_ref, *, own, rank):
    peers_, rows_, lanes = second_ref.shape
    shards = out_ref.shape[0]
    block = tokens_ref.shape[0] // shards
    step = block // 4
    second = second_ref[...]
    sums = jnp.sum(second, axis=0)
    flat = second.reshape(peers_ * rows_, lanes)
    p = jnp.where(lane_group(flat.shape, rank) == 0, flat, 0.0)
    total = jnp.zeros((shards * step, lanes), f32)
    tokens = tokens_ref[...].reshape(shards, 4, step, -1)
    for i in range(4):
        at = pltpu.roll(p, i * rank, 1) if i else p
        high = at.astype(bf16)
        low = (at - high.astype(f32)).astype(bf16)
        part = tokens[:, i].reshape(shards * step, -1)
        total = total + dot(part, high, ((1,), (0,))) + dot(part, low, ((1,), (0,)))
    out_ref[:, :own] = jnp.broadcast_to(sums[None], (shards, own, lanes))
    out_ref[:, own:] = total.reshape(shards, step, lanes)
    pltpu.sync_copy(out_ref, hbm_ref)


def key_products(
    tokens_ref, base_ref, first_ref, its_ref,
    left_ref, right_ref, kept_ref, full_ref, sent, keep, sems,
):
    y0, core = lax.axis_index("y0"), lax.axis_index("core")
    mine = first_ref[:, its_ref.shape[1] :].astype(f32)
    other = its_ref[...].astype(f32)
    pairs = jnp.concatenate(
        [
            jnp.where(core == 0, mine, other)[:, None],
            jnp.where(core == 0, other, mine)[:, None],
        ],
        axis=1,
    )
    momentum = pairs.reshape(base_ref.shape[1], base_ref.shape[0]).T
    full_ref[...] = momentum.astype(bf16)
    settled = (base_ref[...].astype(f32) - own_mom * momentum).astype(bf16)
    groups, block, cols = keep.shape[0] // 2, keep.shape[1], keep.shape[2]
    half = cols // 2

    def product(i, parity):
        at = pl.multiple_of((2 * i + parity) * 2 * block, 2 * block)
        part = dot(tokens_ref[pl.ds(at, 2 * block)], settled, ((1,), (0,)))
        return part.reshape(2, block, cols)

    for i in range(groups):
        sent[2 * i : 2 * i + 2] = product(i, 1 - y0).astype(bf16)
    copies = [
        pltpu.make_async_copy(sent.at[:, :, :half], left_ref, sems.at[0]),
        pltpu.make_async_copy(sent.at[:, :, half:], right_ref, sems.at[1]),
        pltpu.make_async_copy(
            keep, kept_ref.at[: keep.shape[0]], sems.at[2]
        ),
    ]
    for copy in copies[:2]:
        copy.start()
    for i in range(groups):
        keep[2 * i : 2 * i + 2] = product(i, y0)
    copies[2].start()
    for copy in copies:
        copy.wait()


def fold(*refs, stage):
    y2, y1, xl = (lax.axis_index(a) for a in ("y2", "y1", "xl"))
    if stage == 2:
        blocks = [(2 * q + 1 - xl,) for q in range(4)]
    elif stage == 3:
        blocks = [(4 * h + 2 * (1 - y1) + xl, 2 * h + 1 - y1) for h in range(2)]
    else:
        blocks = [
            (4 * h + 2 * y1 + xl, 2 * h + y1, h) for h in (1 - y2, y2)
        ]
    n = stage + 1
    given, outs = refs[:n], refs[n : -(n + 2)]
    held, sent, sems = refs[-(n + 2) : -2], refs[-2], refs[-1]
    kept, left, right, *later = held
    half = left.shape[-1]

    def loads(i):
        at = (blocks[i][0],) * 2 + blocks[i]
        return [
            pltpu.make_async_copy(ref.at[j], buf.at[i], sems.at[i * n + k])
            for k, (ref, buf, j) in enumerate(zip(given, held, at))
        ]

    waits = [loads(i) for i in range(len(blocks))]
    for each in waits:
        for load in each:
            load.start()
    last = len(blocks) * n
    stores = []
    for i, each in enumerate(waits):
        for load in each:
            load.wait()
        for came, at in ((left, slice(0, half)), (right, slice(half, 2 * half))):
            total = kept[i, :, at] + came[i].astype(f32)
            for more in later:
                total = total + more[i, :, at].astype(f32)
            if i < outs[0].shape[0]:
                sent[i, :, at] = total.astype(bf16)
            else:
                outs[1][:, at] = total
        if i < outs[0].shape[0]:
            stores.append(
                pltpu.make_async_copy(sent.at[i], outs[0].at[i], sems.at[last + i])
            )
            stores[-1].start()
    for store in stores:
        store.wait()


def fold_call(stage, kept, *came):
    count = {2: 4, 3: 2, 4: 1}[stage]
    block, cols = kept.shape[1:]
    hbm = pl.BlockSpec(memory_space=pltpu.HBM)
    shape = jax.ShapeDtypeStruct
    out_shape, out_specs = (shape((count, block, cols), bf16),), (hbm,)
    if stage == 4:
        out_shape += (shape((block, cols), f32),)
        out_specs += (pl.BlockSpec(memory_space=pltpu.VMEM),)
    number = max(count, 2)
    given = (kept, *came)
    return pl.pallas_call(
        functools.partial(fold, stage=stage),
        out_shape=out_shape,
        in_specs=[hbm] * len(given),
        out_specs=out_specs,
        scratch_shapes=(
            *[pltpu.VMEM((number, *a.shape[1:]), a.dtype) for a in given],
            pltpu.VMEM((count, block, cols), bf16),
            pltpu.SemaphoreType.DMA((number * (len(given) + 1),)),
        ),
        cost_estimate=pl.CostEstimate(
            flops=count * block * cols, bytes_accessed=8 * count * block * cols,
            transcendentals=0,
        ),
    )(*given)


def shard_sums(third_ref, hbm_ref, total_ref, copies_ref):
    total = jnp.sum(third_ref[...], axis=0)
    total_ref[...] = total
    copies_ref[...] = jnp.broadcast_to(
        total[None, : copies_ref.shape[1]], copies_ref.shape
    )
    pltpu.sync_copy(copies_ref, hbm_ref)


def bases(total_ref, second_ref, basis_ref, token_ref, inverse_ref, *, own, rank):
    total = total_ref[...]
    lanes = total.shape[1]
    sums, token_sum = total[:own], total[own:]
    left = jnp.concatenate(
        [pltpu.roll(sums, lanes - rank, 1), pltpu.roll(sums, lanes - 2 * rank, 1)], axis=0
    )
    row = lax.broadcasted_iota(jnp.int32, (rank, lanes), 0)
    lane = lax.broadcasted_iota(jnp.int32, (rank, lanes), 1)
    work = jnp.where(lane < rank, left, jnp.where(lane == row + rank, 1.0, 0.0))
    for j in range(rank - 1):
        ratio = work[:, j : j + 1] / work[j : j + 1, j : j + 1]
        work = work - jnp.where(row > j, ratio * work[j : j + 1], 0.0)
    pivot = jnp.sum(jnp.where(lane == row, work, 0.0), axis=1, keepdims=True)
    work = jnp.where((lane >= rank) & (lane < 2 * rank), work / jnp.sqrt(pivot), 0.0)
    rest = jnp.zeros((lanes - rank, lanes), f32)
    at = [
        jnp.concatenate([pltpu.roll(work, ((i - 1) * rank) % lanes, 1), rest], axis=0)
        for i in (0, 2, 3)
    ]
    at.insert(1, jnp.concatenate([work, rest], axis=0))
    flat = second_ref[...].reshape(-1, lanes)
    basis_ref[...] = dot(flat, at[0], ((1,), (1,)), highest)
    token_ref[...] = jnp.concatenate(
        [dot(token_sum, a, ((1,), (1,)), highest) for a in at], axis=0
    )
    inverse_ref[...] = at[3]


def outputs(
    fourth_ref, inverse_ref, basis_ref, token_ref, local_ref, base_ref, error_ref,
    full_ref, momentum_ref, base_out, momentum_out, error_out, key_out, q_scratch,
):
    last = ((1,), (1,))
    rows_, cols = base_ref.shape[0], momentum_ref.shape[0]
    flat = fourth_ref[...].reshape(-1, fourth_ref.shape[2])
    q = dot(flat, inverse_ref[...], last, highest)
    q_scratch[...] = q
    key_out[...] = own_upd * dot(token_ref[...], q, last, highest)
    at = lax.axis_index(chips + ("core",)) * cols
    own_q = q_scratch[pl.ds(pl.multiple_of(at, cols), cols)]
    momentum_out[...] = (
        outer_mu * momentum_ref[...].astype(f32)
        + dot(own_q, basis_ref[...], last, highest)
    ).astype(bf16)
    step = rows_ // 4
    for i in range(4):
        here = slice(i * step, (i + 1) * step)
        update = dot(basis_ref[here], q, last, highest)
        base = base_ref[here].astype(f32)
        pseudo = base - local_ref[here].astype(f32) + error_ref[here].astype(f32)
        error_out[here] = (pseudo - update).astype(bf16)
        moment = outer_mu * full_ref[here].astype(f32) + update
        base_out[here] = (base - outer_rate * (outer_mu * moment + update)).astype(bf16)


def in_vmem(kernel, out_shape, n, mib, flops, scratch=(), far=0):
    whole = pl.BlockSpec(memory_space=pltpu.VMEM)
    hbm = pl.BlockSpec(memory_space=pltpu.HBM)
    return pl.pallas_call(
        kernel,
        out_shape=out_shape,
        in_specs=[whole] * n,
        out_specs=tuple(hbm if i < far else whole for i in range(len(out_shape))),
        scratch_shapes=scratch,
        cost_estimate=pl.CostEstimate(
            flops=flops, bytes_accessed=flops // 100, transcendentals=0
        ),
        compiler_params=pltpu.CompilerParams(vmem_limit_bytes=(mib << 20) or None),
    )


def on_device(local_weights, outer_base, momentum, error_feedback, q_start, tokens):
    replicas, shards = lax.axis_size(peers), lax.axis_size(shard)
    rows, kv = outer_base.shape
    rank = q_start.shape[1]
    own = rows // replicas
    cols = kv // replicas
    core = lax.axis_index("core")
    own_tokens = tokens[0]
    block = own_tokens.shape[0] // shards
    shape = jax.ShapeDtypeStruct

    pseudo = (
        outer_base.astype(f32)
        - local_weights[0].astype(f32)
        + error_feedback[0].astype(f32)
    ).reshape(2, rows // 2, kv)
    core = lax.axis_index("core")
    pair = swap(lax.dynamic_index_in_dim(pseudo, 1 - core, 0, False), "core")
    pair = (lax.dynamic_index_in_dim(pseudo, core, 0, False) + pair).astype(bf16)
    first = exchange(
        jnp.concatenate(
            [
                pair.reshape(replicas // 2, own, kv),
                jnp.broadcast_to(momentum.T, (replicas // 2, cols, rows)),
            ],
            axis=1,
        ),
        chips,
    )
    lanes = 4 * rank
    (second,) = in_vmem(
        functools.partial(moments, own=own, rank=rank, replicas=replicas),
        (shape((replicas, own, lanes), f32),),
        2,
        6,
        40000000,
        (pltpu.VMEM((replicas, own, lanes), f32),),
        1,
    )(first, q_start.T)
    second = exchange(second, peers)

    its_momentum = swap(first[:, own:], "core")

    part = (shards // 2, block, kv // 2)
    whole = (*part[:2], kv)
    roomy = shape((2 * part[0], *whole[1:]), f32)
    left, right, kept, full_momentum = in_vmem(
        key_products,
        (shape(part, bf16), shape(part, bf16), roomy, shape((rows, kv), bf16)),
        4,
        16,
        2 * tokens.shape[1] * rows * kv,
        (
            pltpu.VMEM(whole, bf16),
            pltpu.VMEM(whole, f32),
            pltpu.SemaphoreType.DMA((3,)),
        ),
        3,
    )(own_tokens, outer_base, first, its_momentum)
    across = ("y2", "y1", "y0")
    left = lax.ppermute(left, across, [(i, i ^ 1) for i in range(8)])
    right = lax.ppermute(
        right, across, [(i, (i + 1 if i % 2 else i - 1) % 8) for i in range(8)]
    )
    came = [left, right]
    for stage, axis in ((2, "xl"), (3, "y1"), (4, "y2")):
        send, *key_sum = fold_call(stage, kept, *came)
        came.append(swap(send, axis))

    tall = (shards, own + block // 4, lanes)
    (third,) = in_vmem(
        functools.partial(token_products, own=own, rank=rank),
        (shape(tall, f32),),
        2,
        12,
        500000000,
        (pltpu.VMEM(tall, f32),),
        1,
    )(second, own_tokens)
    third = exchange(third, shard)
    copies, total = in_vmem(
        shard_sums,
        (shape((replicas, own, lanes), f32), shape(third.shape[1:], f32)),
        1,
        4,
        1000000,
        (pltpu.VMEM((replicas, own, lanes), f32),),
        1,
    )(third)
    fourth = exchange(copies, peers)
    basis, token_basis, inverse = in_vmem(
        functools.partial(bases, own=own, rank=rank),
        (
            shape((rows, lanes), f32),
            shape((block, lanes), f32),
            shape((lanes, lanes), f32),
        ),
        2,
        6,
        100000000,
    )(total, second)
    new_base, new_momentum, new_error, key_low = in_vmem(
        outputs,
        (
            shape((rows, kv), bf16),
            shape((cols, rows), bf16),
            shape((rows, kv), bf16),
            shape((block, kv), f32),
        ),
        9,
        12,
        400000000,
        (pltpu.VMEM((kv, lanes), f32),),
    )(
        fourth,
        inverse,
        basis,
        token_basis,
        local_weights[0],
        outer_base,
        error_feedback[0],
        full_momentum,
        momentum.T,
    )
    key_rows = (key_sum[0] + came[-1][0].astype(f32) - key_low).astype(bf16)
    return new_base, new_momentum.T, new_error[None], key_rows[None]


def solution(mesh):
    fine = Mesh(
        mesh.devices.reshape(8, 2, 2, 2, 2, 2, 2), chips + ("core",) + shard
    )
    replica = chips + ("core",)
    in_specs = (
        P(replica, shard, None),
        P(shard, None),
        P(shard, replica),
        P(replica, shard, None),
        P(),
        P(replica, None, shard),
    )
    out_specs = (
        P(shard, None),
        P(shard, replica),
        P(replica, shard, None),
        P(replica, shard, None),
    )

    def step(*arrays):
        return on_device(*arrays)

    step = jax.shard_map(
        step, mesh=fine, in_specs=in_specs, out_specs=out_specs, check_vma=False
    )
    return step
```

```python
import functools

import jax
import jax.numpy as jnp
from jax import lax
from jax.experimental import pallas as pl
from jax.experimental.pallas import tpu as pltpu
from jax.sharding import Mesh, PartitionSpec as P


outer_mu = 0.9
outer_rate = 0.7
own_mom = outer_rate * outer_mu * outer_mu
own_upd = outer_rate * (outer_mu + 1.0)


chips = ("z", "xh")
peers = ("core", "z", "xh")
shard = ("y2", "y1", "y0", "xl")
f32, bf16 = jnp.float32, jnp.bfloat16
highest = lax.Precision.HIGHEST


def swap(x, axis):
    return lax.ppermute(x, axis, [(0, 1), (1, 0)])


def exchange(x, axis):
    return lax.all_to_all(x, axis, 0, 0, tiled=True)


def copy_for_each(x, axis):
    return exchange(jnp.broadcast_to(x, (lax.axis_size(axis), *x.shape)), axis)


def dot(a, b, dims, precision=None):
    return lax.dot_general(
        a, b, (dims, ((), ())), precision=precision, preferred_element_type=f32
    )


def lane_group(shape, rank):
    return lax.broadcasted_iota(jnp.int32, shape, 1) // rank


def moments(first_ref, q_ref, hbm_ref, out_ref, *, own, rank, replicas):
    mean = jnp.sum(first_ref[...].astype(f32), axis=0) * (1.0 / replicas)
    q = jnp.concatenate([q_ref[...]] * 4, axis=0)
    p = dot(mean, q, ((1,), (1,)), highest)
    group = lane_group(p.shape, rank)
    p_at = [jnp.where(group == i, p, 0.0) for i in range(4)]
    upper = dot(p_at[0], p_at[1], ((0,), (0,)), highest)
    lower = dot(p_at[0], p_at[2], ((0,), (0,)), highest)
    same = p_at[0] + upper[:own] + lower[own : 2 * own]
    q_rows = dot(mean, p_at[3], ((0,), (0,)), highest)
    out_ref[...] = q_rows.reshape(out_ref.shape) + same[None]
    pltpu.sync_copy(out_ref, hbm_ref)


def token_products(second_ref, tokens_ref, hbm_ref, out_ref, *, own, rank):
    peers_, rows_, lanes = second_ref.shape
    shards = out_ref.shape[0]
    block = tokens_ref.shape[0] // shards
    step = block // 4
    second = second_ref[...]
    sums = jnp.sum(second, axis=0)
    flat = second.reshape(peers_ * rows_, lanes)
    p = jnp.where(lane_group(flat.shape, rank) == 0, flat, 0.0)
    total = jnp.zeros((shards * step, lanes), f32)
    tokens = tokens_ref[...].reshape(shards, 4, step, -1)
    for i in range(4):
        at = pltpu.roll(p, i * rank, 1) if i else p
        high = at.astype(bf16)
        low = (at - high.astype(f32)).astype(bf16)
        part = tokens[:, i].reshape(shards * step, -1)
        total = total + dot(part, high, ((1,), (0,))) + dot(part, low, ((1,), (0,)))
    out_ref[:, :own] = jnp.broadcast_to(sums[None], (shards, own, lanes))
    out_ref[:, own:] = total.reshape(shards, step, lanes)
    pltpu.sync_copy(out_ref, hbm_ref)


def pseudo_halves(
    local_hbm, base_hbm, error_hbm, send_ref, keep_ref, local_ref, base_ref, error_ref, sems
):
    core = lax.axis_index("core")
    half = keep_ref.shape[0]
    pairs = ((local_hbm, local_ref), (base_hbm, base_ref), (error_hbm, error_ref))
    for i, (src, dst) in enumerate(pairs):
        pltpu.make_async_copy(src, dst, sems.at[i]).start()
    for i, (src, dst) in enumerate(pairs):
        pltpu.make_async_copy(src, dst, sems.at[i]).wait()

    def pseudo(which):
        at = pl.ds(pl.multiple_of(which * half, half), half)
        base, local = base_ref[at].astype(f32), local_ref[at].astype(f32)
        return base - local + error_ref[at].astype(f32)

    send_ref[...] = pseudo(1 - core)
    keep_ref[...] = pseudo(core)


def key_products(
    tokens_ref, base_ref, my_ref, its_ref,
    left_ref, right_ref, kept_ref, full_ref, sent, keep, sems,
):
    y0, core = lax.axis_index("y0"), lax.axis_index("core")
    mine = my_ref[...].astype(f32)
    other = its_ref[...].astype(f32)
    pairs = jnp.concatenate(
        [
            jnp.where(core == 0, mine, other)[:, None],
            jnp.where(core == 0, other, mine)[:, None],
        ],
        axis=1,
    )
    momentum = pairs.reshape(base_ref.shape[1], base_ref.shape[0]).T
    full_ref[...] = momentum.astype(bf16)
    settled = (base_ref[...].astype(f32) - own_mom * momentum).astype(bf16)
    groups, block, cols = keep.shape[0] // 2, keep.shape[1], keep.shape[2]
    half = cols // 2

    def product(i, parity):
        at = pl.multiple_of((2 * i + parity) * 2 * block, 2 * block)
        part = dot(tokens_ref[pl.ds(at, 2 * block)], settled, ((1,), (0,)))
        return part.reshape(2, block, cols)

    for i in range(groups):
        sent[2 * i : 2 * i + 2] = product(i, 1 - y0).astype(bf16)
    copies = [
        pltpu.make_async_copy(sent.at[:, :, :half], left_ref, sems.at[0]),
        pltpu.make_async_copy(sent.at[:, :, half:], right_ref, sems.at[1]),
        pltpu.make_async_copy(keep, kept_ref, sems.at[2]),
    ]
    for copy in copies[:2]:
        copy.start()
    for i in range(groups):
        keep[2 * i : 2 * i + 2] = product(i, y0)
    copies[2].start()
    for copy in copies:
        copy.wait()


def fold(*refs, axis, n):
    came_ref, kept_ref, send_ref, keep_ref = refs[:n], refs[n], refs[n + 1], refs[n + 2]
    came, held, sent, sems = refs[n + 3 : 2 * n + 3], *refs[2 * n + 3 :]
    me = lax.axis_index(axis)
    halves = (1 - me, me)
    loads = [
        [
            pltpu.make_async_copy(
                src.at[:, half], dst.at[:, i], sems.at[i * (n + 1) + j]
            )
            for j, (src, dst) in enumerate(zip((*came_ref, kept_ref), (*came, held)))
        ]
        for i, half in enumerate(halves)
    ]
    for load in loads[0] + loads[1]:
        load.start()
    out = [
        pltpu.make_async_copy(sent, send_ref, sems.at[2 * n + 2]),
        pltpu.make_async_copy(held.at[:, 1], keep_ref, sems.at[2 * n + 3]),
    ]
    for i in range(2):
        for load in loads[i]:
            load.wait()
        at, width = 0, held.shape[-1] // n
        for part in came:
            here = slice(at, at + width)
            total = held[:, i, :, here] + part[:, i].astype(f32)
            if i == 0:
                sent[:, :, here] = total.astype(bf16)
            else:
                held[:, i, :, here] = total
            at += width
        out[i].start()
    for copy in out:
        copy.wait()


def fold_call(came, kept, axis):
    groups, _, block, cols = kept.shape
    n = len(came)
    hbm = pl.BlockSpec(memory_space=pltpu.HBM)
    shape = jax.ShapeDtypeStruct
    return pl.pallas_call(
        functools.partial(fold, axis=axis, n=n),
        out_shape=(
            shape((groups, block, cols), bf16),
            shape((groups, block, cols), f32),
        ),
        in_specs=[hbm] * (n + 1),
        out_specs=(hbm, hbm),
        scratch_shapes=(
            *[pltpu.VMEM(c.shape, bf16) for c in came],
            pltpu.VMEM(kept.shape, f32),
            pltpu.VMEM((groups, block, cols), bf16),
            pltpu.SemaphoreType.DMA((2 * n + 4,)),
        ),
        cost_estimate=pl.CostEstimate(
            flops=kept.size, bytes_accessed=kept.size * 6, transcendentals=0
        ),
    )(*came, kept)


def shard_sums(third_ref, hbm_ref, total_ref, copies_ref):
    total = jnp.sum(third_ref[...], axis=0)
    total_ref[...] = total
    copies_ref[...] = jnp.broadcast_to(
        total[None, : copies_ref.shape[1]], copies_ref.shape
    )
    pltpu.sync_copy(copies_ref, hbm_ref)


def bases(total_ref, second_ref, basis_ref, token_ref, inverse_ref, *, own, rank):
    total = total_ref[...]
    lanes = total.shape[1]
    sums, token_sum = total[:own], total[own:]
    left = jnp.concatenate(
        [pltpu.roll(sums, lanes - rank, 1), pltpu.roll(sums, lanes - 2 * rank, 1)], axis=0
    )
    row = lax.broadcasted_iota(jnp.int32, (rank, lanes), 0)
    lane = lax.broadcasted_iota(jnp.int32, (rank, lanes), 1)
    work = jnp.where(lane < rank, left, jnp.where(lane == row + rank, 1.0, 0.0))
    for j in range(rank - 1):
        ratio = work[:, j : j + 1] / work[j : j + 1, j : j + 1]
        work = work - jnp.where(row > j, ratio * work[j : j + 1], 0.0)
    pivot = jnp.sum(jnp.where(lane == row, work, 0.0), axis=1, keepdims=True)
    work = jnp.where((lane >= rank) & (lane < 2 * rank), work / jnp.sqrt(pivot), 0.0)
    rest = jnp.zeros((lanes - rank, lanes), f32)
    at = [
        jnp.concatenate([pltpu.roll(work, ((i - 1) * rank) % lanes, 1), rest], axis=0)
        for i in (0, 2, 3)
    ]
    at.insert(1, jnp.concatenate([work, rest], axis=0))
    flat = second_ref[...].reshape(-1, lanes)
    basis_ref[...] = dot(flat, at[0], ((1,), (1,)), highest)
    token_ref[...] = jnp.concatenate(
        [dot(token_sum, a, ((1,), (1,)), highest) for a in at], axis=0
    )
    inverse_ref[...] = at[3]


def outputs(
    fourth_ref, inverse_ref, basis_ref, token_ref, local_ref, base_ref, error_ref,
    full_ref, momentum_ref, base_out, momentum_out, error_out, key_out, q_scratch,
):
    last = ((1,), (1,))
    rows_, cols = base_ref.shape[0], momentum_ref.shape[0]
    flat = fourth_ref[...].reshape(-1, fourth_ref.shape[2])
    q = dot(flat, inverse_ref[...], last, highest)
    q_scratch[...] = q
    key_out[...] = own_upd * dot(token_ref[...], q, last, highest)
    at = lax.axis_index(chips + ("core",)) * cols
    own_q = q_scratch[pl.ds(pl.multiple_of(at, cols), cols)]
    momentum_out[...] = (
        outer_mu * momentum_ref[...].astype(f32)
        + dot(own_q, basis_ref[...], last, highest)
    ).astype(bf16)
    step = rows_ // 4
    for i in range(4):
        here = slice(i * step, (i + 1) * step)
        update = dot(basis_ref[here], q, last, highest)
        base = base_ref[here].astype(f32)
        pseudo = base - local_ref[here].astype(f32) + error_ref[here].astype(f32)
        error_out[here] = (pseudo - update).astype(bf16)
        moment = outer_mu * full_ref[here].astype(f32) + update
        base_out[here] = (base - outer_rate * (outer_mu * moment + update)).astype(bf16)


def in_vmem(kernel, out_shape, n, mib, flops, scratch=(), far=0, far_in=False):
    whole = pl.BlockSpec(memory_space=pltpu.VMEM)
    hbm = pl.BlockSpec(memory_space=pltpu.HBM)
    return pl.pallas_call(
        kernel,
        out_shape=out_shape,
        in_specs=[hbm if far_in else whole] * n,
        out_specs=tuple(hbm if i < far else whole for i in range(len(out_shape))),
        scratch_shapes=scratch,
        cost_estimate=pl.CostEstimate(
            flops=flops, bytes_accessed=flops // 100, transcendentals=0
        ),
        compiler_params=pltpu.CompilerParams(vmem_limit_bytes=(mib << 20) or None),
    )


def on_device(local_weights, outer_base, momentum, error_feedback, q_start, tokens):
    replicas, shards = lax.axis_size(peers), lax.axis_size(shard)
    rows, kv = outer_base.shape
    rank = q_start.shape[1]
    own = rows // replicas
    cols = kv // replicas
    own_tokens = tokens[0]
    block = own_tokens.shape[0] // shards
    shape = jax.ShapeDtypeStruct

    my_momentum = copy_for_each(momentum.T, chips)
    half = shape((rows // 2, kv), f32)
    given = pltpu.VMEM((rows, kv), bf16)
    send, pair = in_vmem(
        pseudo_halves,
        (half, half),
        3,
        8,
        1000000,
        (given, given, given, pltpu.SemaphoreType.DMA((3,))),
        far_in=True,
    )(local_weights[0], outer_base, error_feedback[0])
    send = swap(send, "core")
    pair = (pair + send).astype(bf16)
    pair, my_momentum = lax.optimization_barrier((pair, my_momentum))
    first = exchange(pair.reshape(replicas // 2, own, kv), chips)
    lanes = 4 * rank
    (second,) = in_vmem(
        functools.partial(moments, own=own, rank=rank, replicas=replicas),
        (shape((replicas, own, lanes), f32),),
        2,
        6,
        40000000,
        (pltpu.VMEM((replicas, own, lanes), f32),),
        1,
    )(first, q_start.T)
    second = exchange(second, peers)

    its_momentum = swap(my_momentum, "core")

    part = (shards // 2, block, kv // 2)
    whole = (*part[:2], kv)
    left, right, kept, full_momentum = in_vmem(
        key_products,
        (shape(part, bf16), shape(part, bf16), shape(whole, f32), shape((rows, kv), bf16)),
        4,
        0,
        2 * tokens.shape[1] * rows * kv,
        (
            pltpu.VMEM(whole, bf16),
            pltpu.VMEM(whole, f32),
            pltpu.SemaphoreType.DMA((3,)),
        ),
        3,
    )(own_tokens, outer_base, my_momentum, its_momentum)
    across = ("y2", "y1", "y0")
    left = lax.ppermute(left, across, [(i, i ^ 1) for i in range(8)])
    right = lax.ppermute(
        right, across, [(i, (i + 1 if i % 2 else i - 1) % 8) for i in range(8)]
    )
    for axis, groups, came in (
        ("xl", 4, (left, right)), ("y1", 2, None), ("y2", 1, None)
    ):
        view = (groups, 2, block)
        send, kept = fold_call(
            [c.reshape(*view, -1) for c in came or (send,)],
            kept.reshape(*view, kv),
            axis,
        )
        send = swap(send, axis)

    tall = (shards, own + block // 4, lanes)
    (third,) = in_vmem(
        functools.partial(token_products, own=own, rank=rank),
        (shape(tall, f32),),
        2,
        12,
        500000000,
        (pltpu.VMEM(tall, f32),),
        1,
    )(second, own_tokens)
    third = exchange(third, shard)
    copies, total = in_vmem(
        shard_sums,
        (shape((replicas, own, lanes), f32), shape(third.shape[1:], f32)),
        1,
        4,
        1000000,
        (pltpu.VMEM((replicas, own, lanes), f32),),
        1,
    )(third)
    fourth = exchange(copies, peers)
    basis, token_basis, inverse = in_vmem(
        functools.partial(bases, own=own, rank=rank),
        (
            shape((rows, lanes), f32),
            shape((block, lanes), f32),
            shape((lanes, lanes), f32),
        ),
        2,
        6,
        100000000,
    )(total, second)
    new_base, new_momentum, new_error, key_low = in_vmem(
        outputs,
        (
            shape((rows, kv), bf16),
            shape((cols, rows), bf16),
            shape((rows, kv), bf16),
            shape((block, kv), f32),
        ),
        9,
        12,
        400000000,
        (pltpu.VMEM((kv, lanes), f32),),
    )(
        fourth,
        inverse,
        basis,
        token_basis,
        local_weights[0],
        outer_base,
        error_feedback[0],
        full_momentum,
        momentum.T,
    )
    key_rows = (kept[0] + send[0].astype(f32) - key_low).astype(bf16)
    return new_base, new_momentum.T, new_error[None], key_rows[None]


def solution(mesh):
    fine = Mesh(
        mesh.devices.reshape(8, 2, 2, 2, 2, 2, 2), chips + ("core",) + shard
    )
    replica = chips + ("core",)
    in_specs = (
        P(replica, shard, None),
        P(shard, None),
        P(shard, replica),
        P(replica, shard, None),
        P(),
        P(replica, None, shard),
    )
    out_specs = (
        P(shard, None),
        P(shard, replica),
        P(replica, shard, None),
        P(replica, shard, None),
    )

    def step(*arrays):
        return on_device(*arrays)

    step = jax.shard_map(
        step, mesh=fine, in_specs=in_specs, out_specs=out_specs, check_vma=False
    )
    return step
```
